512 devices in a mesh: dp: 128 (over y, x, z_hi, core), mp: 4 (over z_lo).
Axes of the slice: x: 4, y: 4, z: 16 (z_hi: 4, z_lo: 4; z = z_hi * 4 + z_lo), core: 2. Of those that a mesh axis runs over, the one named last changes fastest.
Arguments:
- layer_input: bfloat16 [512, 8192], P('dp'), may hold values from -6 to 6
- pre_act: bfloat16 [512, 8192], P('dp', 'mp'), may hold values from -8 to 8
- hidden_adjoint: bfloat16 [512, 8192], P('dp', 'mp'), may hold values from -6 to 6
- output_adjoint: bfloat16 [512, 8192], P('dp', 'mp'), may hold values from -6 to 6
Outputs:
- precond_in: float32 [8192, 8192], P('dp', 'mp')
- direction_in: float32 [8192, 8192], P('dp', 'mp')
- precond_out: float32 [8192, 8192], P('dp', 'mp')
- direction_out: float32 [8192, 8192], P('dp', 'mp')
- sq_norm: float32 [], replicated
The draws below stay inside these ranges and needn't reach their ends.
All inputs are finite; a program needn't handle non-finite values.
Results may differ from the reference program's by a relative error of at most 0.0029.
Values may be sent and summed in bfloat16 or wider, within the bound.
A program may use at most 64 MiB of HBM per device.

```python
import jax
import jax.numpy as jnp

D = 8192
H = 8192
EXAMPLES = 512


def shard_levels(stream_key, dims, cuts, low, top_value):
    loudness, own = 1.0, jax.random.fold_in(stream_key, 6)
    for dim, blocks in cuts:
        draws = jnp.exp(jax.random.uniform(jax.random.fold_in(own, dim), (blocks,), jnp.float32, low / len(cuts), top_value / len(cuts)))
        loudness = loudness * jnp.repeat(draws, dims[dim] // blocks).reshape([-1 if axis == dim else 1 for axis in range(len(dims))])
    return loudness


def scatter_about(stream_key, dims, scale, limit, cuts=(), held_as=jnp.bfloat16):
    loudness = shard_levels(stream_key, dims, cuts, -0.22, 0.18) if cuts else 1.0
    result = jax.random.normal(stream_key, dims, jnp.float32) * scale * loudness
    return jnp.minimum(jnp.maximum(result, -limit), limit).astype(held_as)


def setup_inputs(seed: int = 0) -> dict:
    arg_keys = jax.random.split(jax.random.key(seed), 5)
    return {
        "layer_input": scatter_about(arg_keys[0], (EXAMPLES, D), 1.0, 6.0, ((0, 128),)),
        "pre_act": scatter_about(arg_keys[1], (EXAMPLES, H), 1.5, 8.0, ((0, 128), (1, 4))),
        "hidden_adjoint": scatter_about(arg_keys[2], (EXAMPLES, H), 1.0, 6.0, ((0, 128), (1, 4))),
        "output_adjoint": scatter_about(arg_keys[3], (EXAMPLES, D), 1.0, 6.0, ((0, 128), (1, 4))),
    }


DAMPING = 0.1
EXPONENT = 0.75

def square_bf(values):
    wide = values.astype(jnp.float32)
    return (wide * wide).astype(jnp.bfloat16)

def layer_stats(activation, adjoint, total_rows):
    gradient = jnp.dot(activation.T, adjoint, preferred_element_type=jnp.float32) / total_rows
    squares = jnp.dot(square_bf(activation).T, square_bf(adjoint), preferred_element_type=jnp.float32) / total_rows
    precond = (squares + DAMPING) ** EXPONENT
    return (gradient, precond)

def reference(layer_input, pre_act, hidden_adjoint, output_adjoint):
    total_rows = layer_input.shape[0]
    preact = pre_act.astype(jnp.float32)
    logistic = jax.nn.sigmoid(preact)
    hidden = (preact * logistic).astype(jnp.bfloat16)
    adjoint = (hidden_adjoint.astype(jnp.float32) * logistic * (1.0 + preact * (1.0 - logistic))).astype(jnp.bfloat16)
    gradient_in, precond_in = layer_stats(layer_input, adjoint, total_rows)
    gradient_out, precond_out = layer_stats(hidden, output_adjoint, total_rows)
    sq_norm = jnp.sum(gradient_in * gradient_in / precond_in) + jnp.sum(gradient_out * gradient_out / precond_out)
    rescale = jnp.sqrt(2.0 * D * H / sq_norm)
    direction_in = gradient_in / precond_in * rescale
    direction_out = gradient_out / precond_out * rescale
    return (precond_in, direction_in, precond_out, direction_out, sq_norm)
```

```python
import jax
import jax.numpy as jnp
from jax import lax
from jax.experimental import pallas as pl
from jax.experimental.pallas import tpu as pltpu
from jax.sharding import Mesh
from jax.sharding import PartitionSpec as P

D = 8192
H = 8192
EXAMPLES = 512
DP = ("dp_0", "dp_1", "dp_2", "dp_3")
AXES = ("dp_0", "dp_1", "dp_2", "dp_3", "mp")
MESH = pl.DeviceIdType.MESH
BF = jnp.bfloat16
F32 = jnp.float32

DAMPING = 0.1
EXPONENT = 0.75

N_PAIR = 1
N_MSG = 128
TILE = 256


def mod4(a):
    return lax.rem(a, 4)


def sq_round(v):
    w = v.astype(F32)
    return (w * w).astype(BF)


def kernel(
    li_hbm, pre_hbm, ha_hbm, oa_hbm,
    p_out, r_out, n_out,
    pre_v, ha_v, oa_v, hid, stack, pair_src, pair_dst, pair_f32,
    big, v1, v2, v3, tile_f32, lhs, lhs_t, lhs_sq, acc_g, acc_s, norm_acc, red_a, red_b,
    in_sem, send_sem, recv_sem, li_send, li_recv, hid_send, hid_recv, red_send, red_recv,
):
    y, x, zh, c, zl = (lax.axis_index(a) for a in AXES)
    d = 1 - c
    f = x * d + y * c
    s = y * d + x * c
    fp, fm, fo = mod4(f + 1), mod4(f + 3), mod4(f + 2)
    sp, sm, so = mod4(s + 1), mod4(s + 3), mod4(s + 2)
    zp, zm, zo = mod4(zh + 1), mod4(zh + 3), mod4(zh + 2)

    def at_f(fd):
        return (y * d + fd * c, fd * d + x * c, zh, c, zl)

    def at_s(sd):
        return (sd * d + y * c, x * d + sd * c, zh, c, zl)

    def at_z(zd):
        return (y, x, zd, c, zl)

    partner = (y, x, zh, d, zl)

    loads = [
        pltpu.make_async_copy(pre_hbm, pre_v, in_sem.at[0]),
        pltpu.make_async_copy(ha_hbm, ha_v, in_sem.at[1]),
        pltpu.make_async_copy(oa_hbm, oa_v, in_sem.at[2]),
    ]
    for load in loads:
        load.start()

    barrier = pltpu.get_barrier_semaphore()

    def hello(device):
        pl.semaphore_signal(barrier, inc=1, device_id=device, device_id_type=MESH)

    hello(partner)
    for k in (1, 2, 3):
        hello((mod4(y + k), x, zh, c, zl))
        hello((y, mod4(x + k), zh, c, zl))
    hello(at_z(zp))
    hello(at_z(zm))
    for ys in range(4):
        own = jnp.logical_and(y == ys, zl == y)

        @pl.when(jnp.logical_not(own))
        def _():
            hello((ys, x, zh, c, y))

    for load in loads:
        load.wait()
    preact = pre_v[...].astype(F32)
    logistic = 1.0 / (1.0 + jnp.exp(-preact))
    hid[...] = (preact * logistic).astype(BF)
    adjoint = (ha_v[...].astype(F32) * logistic * (1.0 + preact * (1.0 - logistic))).astype(BF)
    stack[0:4, :] = adjoint.astype(F32)
    stack[4:8, :] = oa_v[...].astype(F32)
    pair_src[0] = stack[:, 0:1024].astype(BF)
    pair_src[1] = stack[:, 1024:2048].astype(BF)

    pl.semaphore_wait(barrier, 13 - jnp.where(y == zl, 1, 0).astype(jnp.int32))

    sent = []

    def send(src, dst, device):
        i = len(sent)
        copy = pltpu.make_async_remote_copy(
            src_ref=src, dst_ref=dst, send_sem=send_sem.at[i], recv_sem=recv_sem.at[i],
            device_id=device, device_id_type=MESH,
        )
        copy.start()
        sent.append(copy)
        return copy

    exchange = send(pair_src.at[d], pair_dst, partner)

    li_copies = []
    for k in (1, 2, 3):
        yd = mod4(y + k)
        cols = pl.ds(pl.multiple_of(yd * 2048, 2048), 2048)
        copy = pltpu.make_async_remote_copy(
            src_ref=li_hbm.at[:, cols], dst_ref=v1.at[y], send_sem=li_send.at[k - 1],
            recv_sem=li_recv.at[k - 1], device_id=(yd, x, zh, c, zl), device_id_type=MESH,
        )
        copy.start()
        li_copies.append(copy)
    li_own = pltpu.make_async_copy(
        li_hbm.at[:, pl.ds(pl.multiple_of(y * 2048, 2048), 2048)], v1.at[y], in_sem.at[0]
    )
    li_own.start()
    hid_copies = []
    for zd in range(4):
        own = jnp.logical_and(y == zl, zl == zd)
        remote = pltpu.make_async_remote_copy(
            src_ref=hid, dst_ref=v1.at[4 + y], send_sem=hid_send.at[zd],
            recv_sem=hid_recv.at[y], device_id=(zl, x, zh, c, zd), device_id_type=MESH,
        )
        local = pltpu.make_async_copy(hid, v1.at[4 + y], hid_recv.at[y])
        hid_copies.append((own, remote))

        @pl.when(own)
        def _():
            local.start()

        @pl.when(jnp.logical_not(own))
        def _():
            remote.start()

    exchange.wait_recv()
    mine = pair_src[c].astype(F32)
    other = pair_dst[...].astype(F32)
    first = c == 0
    pair_f32[0:8, :] = jnp.where(first, mine, other)
    pair_f32[8:16, :] = jnp.where(first, other, mine)
    big[c, zh, s, f] = pair_f32[...].astype(BF)

    def block(z, sd, fd):
        return big.at[c, z, sd, fd]

    def half(z, sd, fd, k):
        return big.at[c, z, sd, fd, :, pl.ds(512 * k, 512)]

    z1p = send(block(zh, s, f), block(zh, s, f), at_z(zp))
    z1m = send(block(zh, s, f), block(zh, s, f), at_z(zm))

    slices = (zh, zm, zp, zo)
    F1, F2, S1, S2, X = {}, {}, {}, {}, {}

    def both_s(k, j, fd):
        z = slices[k]
        S1[k, j, 0] = send(block(z, s, fd), block(z, s, fd), at_s(sp))
        S1[k, j, 1] = send(block(z, s, fd), block(z, s, fd), at_s(sm))

    def stage_a(k):
        z = slices[k]
        F1[k, 0] = send(block(z, s, f), block(z, s, f), at_f(fp))
        F1[k, 1] = send(block(z, s, f), block(z, s, f), at_f(fm))
        both_s(k, 0, f)

    def stage_b(k):
        z = slices[k]
        F1[k, 0].wait_recv()
        F2[k, 0] = send(half(z, s, fm, 0), half(z, s, fm, 0), at_f(fp))
        F1[k, 1].wait_recv()
        F2[k, 1] = send(half(z, s, fp, 1), half(z, s, fp, 1), at_f(fm))
        both_s(k, 1, fm)
        both_s(k, 2, fp)

    def stage_c(k):
        z = slices[k]
        S1[k, 0, 0].wait_recv()
        S2[k, 0] = send(block(z, sm, f), block(z, sm, f), at_s(sp))

    def stage_d(k):
        F2[k, 0].wait_recv()
        F2[k, 1].wait_recv()
        both_s(k, 3, fo)

    def stage_e(k):
        z = slices[k]
        S1[k, 1, 0].wait_recv()
        S2[k, 1] = send(block(z, sm, fm), block(z, sm, fm), at_s(sp))
        S1[k, 2, 1].wait_recv()
        S2[k, 2] = send(block(z, sp, fp), block(z, sp, fp), at_s(sm))

    def stage_f(k):
        z = slices[k]
        S1[k, 3, 1].wait_recv()
        S2[k, 3] = send(block(z, sp, fo), block(z, sp, fo), at_s(sm))

    def stage_g(k):
        z = slices[k]
        S1[k, 0, 1].wait_recv()
        S1[k, 1, 1].wait_recv()
        S1[k, 2, 0].wait_recv()
        S1[k, 3, 0].wait_recv()
        for j in range(4):
            S2[k, j].wait_recv()
        X[k] = send(big.at[c, z], big.at[c, z], partner)

    def rows_x():
        for copy in li_copies:
            copy.wait_recv()
        li_own.wait()
        for ys in range(4):
            pltpu.make_async_copy(hid, v1.at[4 + ys], hid_recv.at[ys]).wait()
        copies = []
        for k in (1, 2, 3):
            xd = mod4(x + k)
            cols = pl.ds(pl.multiple_of(xd * 512, 512), 512)
            copies.append(send(v1.at[:, :, cols], v2.at[x], (y, xd, zh, c, zl)))
        local = pltpu.make_async_copy(
            v1.at[:, :, pl.ds(pl.multiple_of(x * 512, 512), 512)], v2.at[x], in_sem.at[1]
        )
        local.start()
        return copies, local

    def rows_z(copies, local):
        for copy in copies:
            copy.wait_recv()
        local.wait()
        out = []
        for k in (1, 2, 3):
            zd = mod4(zh + k)
            cols = pl.ds(pl.multiple_of(zd * 128, 128), 128)
            out.append(send(v2.at[:, :, :, cols], v3.at[c, zh], at_z(zd)))
        local = pltpu.make_async_copy(
            v2.at[:, :, :, pl.ds(pl.multiple_of(zh * 128, 128), 128)], v3.at[c, zh], in_sem.at[2]
        )
        local.start()
        return out, local

    def rows_core(copies, local):
        for copy in copies:
            copy.wait_recv()
        local.wait()
        return send(v3.at[c], v3.at[c], partner)

    stage_a(0)
    stage_b(0)
    stage_c(0)
    z1p.wait_recv()
    z2p = send(half(zm, s, f, 0), half(zm, s, f, 0), at_z(zp))
    z1m.wait_recv()
    z2m = send(half(zp, s, f, 1), half(zp, s, f, 1), at_z(zm))
    stage_a(1)
    stage_a(2)
    stage_d(0)
    stage_e(0)
    rows = rows_x()
    stage_b(1)
    stage_b(2)
    stage_c(1)
    stage_c(2)
    stage_f(0)
    stage_d(1)
    stage_d(2)
    z2p.wait_recv()
    z2m.wait_recv()
    stage_a(3)
    rows = rows_z(*rows)
    stage_e(1)
    stage_e(2)
    stage_g(0)
    stage_b(3)
    stage_c(3)
    stage_f(1)
    stage_f(2)
    stage_d(3)
    stage_g(1)
    stage_g(2)
    stage_e(3)
    last_rows = rows_core(*rows)
    stage_f(3)

    last_rows.wait_recv()
    row = lax.broadcasted_iota(jnp.int32, (16, 128), 0)
    lane = lax.broadcasted_iota(jnp.int32, (16, 128), 1)
    kind = lax.rem(row // 4, 2)
    side = lane // 64
    keep = kind == side
    straight = side == c

    @pl.loop(0, 64)
    def _(i):
        z, xs, ys = i // 16, lax.rem(i // 4, 4), lax.rem(i, 4)
        for q in range(4):
            core, kd = divmod(q, 2)
            tile_f32[4 * q : 4 * q + 4, :] = v3[core, z, xs, kd * 4 + ys].astype(F32)
        data = tile_f32[...]
        turned = pltpu.roll(data, 64, 1)
        rows16 = jnp.where(keep, jnp.where(straight, data, turned), 0.0).astype(BF)
        lhs[0, z, ys * 4 + xs] = rows16
        lhs[1, z, xs * 4 + ys] = rows16

    for cc in range(2):
        for z in range(4):
            t = jnp.transpose(lhs[cc, z].reshape(256, 128).astype(F32))
            lhs_t[cc, z] = t.astype(BF)
            lhs_sq[cc, z] = (t * t).astype(BF)

    def dots(cc, z, cols):
        right = big[cc, z, :, :, :, cols].reshape(256, TILE)
        grad = jnp.dot(lhs_t[cc, z], right, preferred_element_type=F32)
        square = jnp.dot(lhs_sq[cc, z], sq_round(right), preferred_element_type=F32)
        return grad, square

    for k in range(3):
        X[k].wait_recv()

    for cc in range(2):

        @pl.loop(0, 1024 // TILE)
        def _(j):
            cols = pl.ds(pl.multiple_of(j * TILE, TILE), TILE)
            wide = pl.ds(pl.multiple_of(cc * 1024 + j * TILE, TILE), TILE)
            parts = [dots(cc, slices[k], cols) for k in range(3)]
            acc_g[:, wide] = parts[0][0] + parts[1][0] + parts[2][0]
            acc_s[:, wide] = parts[0][1] + parts[1][1] + parts[2][1]

    stage_g(3)
    X[3].wait_recv()
    norm_acc[...] = jnp.zeros_like(norm_acc)
    for cc in range(2):

        @pl.loop(0, 1024 // TILE)
        def _(j):
            cols = pl.ds(pl.multiple_of(j * TILE, TILE), TILE)
            wide = pl.ds(pl.multiple_of(cc * 1024 + j * TILE, TILE), TILE)
            grad, square = dots(cc, zo, cols)
            grad = (acc_g[:, wide] + grad) / EXAMPLES
            base = (acc_s[:, wide] + square) / EXAMPLES + DAMPING
            precond = jnp.exp(EXPONENT * jnp.log(base))
            ratio = grad / precond
            p_out[:, wide] = precond
            r_out[:, wide] = ratio
            norm_acc[...] += jnp.sum(grad * ratio, axis=0, keepdims=True)

    own_norm = jnp.sum(norm_acc[...], axis=1, keepdims=True)
    plane = (y * 4 + x) * 2 + c
    red_a[plane] = jnp.broadcast_to(own_norm, (1, 128))

    @pl.loop(1, 32)
    def _(k):
        to = lax.rem(plane + k, 32)
        pltpu.make_async_remote_copy(
            src_ref=red_a.at[plane], dst_ref=red_a.at[plane], send_sem=red_send.at[0],
            recv_sem=red_recv.at[0],
            device_id=(to // 8, lax.rem(to // 2, 4), zh, lax.rem(to, 2), zl), device_id_type=MESH,
        ).start()

    pltpu.make_async_copy(red_a.at[pl.ds(0, 31)], red_a.at[pl.ds(0, 31)], red_recv.at[0]).wait()
    z16 = zh * 4 + zl
    red_b[z16] = jnp.sum(red_a[...], axis=0)

    @pl.loop(1, 16)
    def _(k):
        to = lax.rem(z16 + k, 16)
        pltpu.make_async_remote_copy(
            src_ref=red_b.at[z16], dst_ref=red_b.at[z16], send_sem=red_send.at[1],
            recv_sem=red_recv.at[1],
            device_id=(y, x, to // 4, c, lax.rem(to, 4)), device_id_type=MESH,
        ).start()

    for copy in sent:
        copy.wait_send()
    for copy in li_copies:
        copy.wait_send()
    for own, remote in hid_copies:

        @pl.when(jnp.logical_not(own))
        def _():
            remote.wait_send()

    pltpu.make_async_copy(red_a.at[pl.ds(0, 31)], red_a.at[pl.ds(0, 31)], red_send.at[0]).wait()
    pltpu.make_async_copy(red_b.at[pl.ds(0, 15)], red_b.at[pl.ds(0, 15)], red_recv.at[1]).wait()
    n_out[...] = jnp.sum(red_b[...], axis=0)
    pltpu.make_async_copy(red_b.at[pl.ds(0, 15)], red_b.at[pl.ds(0, 15)], red_send.at[1]).wait()


def shards(layer_input, pre_act, hidden_adjoint, output_adjoint):
    any_space = pl.BlockSpec(memory_space=pl.ANY)
    vmem = pl.BlockSpec(memory_space=pltpu.VMEM)
    dma = pltpu.SemaphoreType.DMA
    precond, ratio, norm = pl.pallas_call(
        kernel,
        out_shape=(
            jax.ShapeDtypeStruct((128, 2048), F32),
            jax.ShapeDtypeStruct((128, 2048), F32),
            jax.ShapeDtypeStruct((1, 128), F32),
        ),
        in_specs=[any_space] * 4,
        out_specs=(vmem, vmem, vmem),
        scratch_shapes=[
            pltpu.VMEM((4, 2048), BF),
            pltpu.VMEM((4, 2048), BF),
            pltpu.VMEM((4, 2048), BF),
            pltpu.VMEM((4, 2048), BF),
            pltpu.VMEM((8, 2048), F32),
            pltpu.VMEM((2, 8, 1024), BF),
            pltpu.VMEM((8, 1024), BF),
            pltpu.VMEM((16, 1024), F32),
            pltpu.VMEM((2, 4, 4, 4, 16, 1024), BF),
            pltpu.VMEM((8, 4, 2048), BF),
            pltpu.VMEM((4, 8, 4, 512), BF),
            pltpu.VMEM((2, 4, 4, 8, 4, 128), BF),
            pltpu.VMEM((16, 128), F32),
            pltpu.VMEM((2, 4, 16, 16, 128), BF),
            pltpu.VMEM((2, 4, 128, 256), BF),
            pltpu.VMEM((2, 4, 128, 256), BF),
            pltpu.VMEM((128, 2048), F32),
            pltpu.VMEM((128, 2048), F32),
            pltpu.VMEM((1, TILE), F32),
            pltpu.VMEM((32, 1, 128), F32),
            pltpu.VMEM((16, 1, 128), F32),
            dma((3,)),
            dma((N_MSG,)),
            dma((N_MSG,)),
            dma((3,)),
            dma((3,)),
            dma((4,)),
            dma((4,)),
            dma((2,)),
            dma((2,)),
        ],
        compiler_params=pltpu.CompilerParams(collective_id=0, has_side_effects=True),
    )(layer_input, pre_act, hidden_adjoint, output_adjoint)
    sq_norm = norm[0, 0]
    rescale = jnp.sqrt(2.0 * D * H / sq_norm)
    return (
        precond[:64],
        ratio[:64] * rescale,
        precond[64:],
        ratio[64:] * rescale,
        sq_norm,
    )


def solution(mesh):
    torus = Mesh(mesh.devices.reshape(4, 4, 4, 2, mesh.shape["mp"]), AXES)
    placed = (P(DP, None), P(DP, "mp"), P(DP, "mp"), P(DP, "mp"))
    return jax.shard_map(
        shards,
        mesh=torus,
        in_specs=placed,
        out_specs=(P(DP, "mp"), P(DP, "mp"), P(DP, "mp"), P(DP, "mp"), P()),
        check_vma=False,
    )
```

```python
import jax
import jax.numpy as jnp
from jax import lax
from jax.experimental import pallas as pl
from jax.experimental.pallas import tpu as pltpu
from jax.sharding import Mesh
from jax.sharding import PartitionSpec as P

D = 8192
H = 8192
EXAMPLES = 512
DP = ("dp_0", "dp_1", "dp_2", "dp_3")
AXES = ("dp_0", "dp_1", "dp_2", "dp_3", "mp")
MESH = pl.DeviceIdType.MESH
BF = jnp.bfloat16
F32 = jnp.float32

DAMPING = 0.1
EXPONENT = 0.75

N_MSG = 128
TILE = 256
K1_LIMIT = 32 * 1024 * 1024


def mod4(a):
    return lax.rem(a, 4)


def sq_round(v):
    w = v.astype(F32)
    return (w * w).astype(BF)


def kernel(
    li_hbm, pre_hbm, ha_hbm, oa_hbm,
    p_all, r_all, n_out,
    pre_v, ha_v, oa_v, li_v, stack, rows0, pair_src, pair_dst,
    big, rows1, rows2, rows3, lhs_t, lhs_sq, acc_g, acc_s, norm_acc, red_a, red_b,
    in_sem, send_sem, recv_sem, out_send, out_recv, red_send, red_recv, hello_sem,
):
    y, x, zh, c, zl = (lax.axis_index(a) for a in AXES)
    d = 1 - c
    f = x * d + y * c
    s = y * d + x * c
    fp, fm, fo = mod4(f + 1), mod4(f + 3), mod4(f + 2)
    sp, sm, so = mod4(s + 1), mod4(s + 3), mod4(s + 2)
    zp, zm, zo = mod4(zh + 1), mod4(zh + 3), mod4(zh + 2)

    def at_f(fd):
        return (y * d + fd * c, fd * d + x * c, zh, c, zl)

    def at_s(sd):
        return (sd * d + y * c, x * d + sd * c, zh, c, zl)

    def at_z(zd):
        return (y, x, zd, c, zl)

    partner = (y, x, zh, d, zl)

    barrier = pltpu.get_barrier_semaphore()

    def tell(semaphore, device):
        pl.semaphore_signal(semaphore, inc=1, device_id=device, device_id_type=MESH)

    tell(barrier, at_z(zp))
    tell(barrier, at_z(zm))
    for k in (1, 2, 3):
        tell(barrier, (y, x, zh, c, mod4(zl + k)))
        tell(barrier, (mod4(y + k), x, zh, c, zl))
        tell(barrier, (y, mod4(x + k), zh, c, zl))
    tell(barrier, partner)

    loads = [
        pltpu.make_async_copy(pre_hbm, pre_v, in_sem.at[0]),
        pltpu.make_async_copy(ha_hbm, ha_v, in_sem.at[1]),
        pltpu.make_async_copy(oa_hbm, oa_v, in_sem.at[2]),
        pltpu.make_async_copy(
            li_hbm.at[:, pl.ds(pl.multiple_of(zl * 2048, 2048), 2048)], li_v, in_sem.at[3]
        ),
    ]
    for load in loads:
        load.start()
    for load in loads:
        load.wait()
    preact = pre_v[...].astype(F32)
    logistic = 1.0 / (1.0 + jnp.exp(-preact))
    hidden = (preact * logistic).astype(BF)
    adjoint = (ha_v[...].astype(F32) * logistic * (1.0 + preact * (1.0 - logistic))).astype(BF)
    stack[0, 0:4, :] = adjoint.astype(F32)
    stack[0, 4:8, :] = oa_v[...].astype(F32)
    stack[1, 0:4, :] = li_v[...].astype(F32)
    stack[1, 4:8, :] = hidden.astype(F32)
    pair_src[0] = stack[0, :, 0:1024].astype(BF)
    pair_src[1] = stack[0, :, 1024:2048].astype(BF)
    for k in range(4):
        rows0[k] = stack[1, :, 512 * k : 512 * (k + 1)].astype(BF)

    pl.semaphore_wait(barrier, 12)

    sent = []

    def send(src, dst, device):
        i = len(sent)
        copy = pltpu.make_async_remote_copy(
            src_ref=src, dst_ref=dst, send_sem=send_sem.at[i], recv_sem=recv_sem.at[i],
            device_id=device, device_id_type=MESH,
        )
        copy.start()
        sent.append(copy)
        return copy

    exchange = send(pair_src.at[d], pair_dst, partner)
    row_hop = []
    for k in (1, 2, 3):
        xd = mod4(x + k)
        row_hop.append(send(rows0.at[xd], rows1.at[x], (y, xd, zh, c, zl)))
    row_own = pltpu.make_async_copy(rows0.at[x], rows1.at[x], in_sem.at[0])
    row_own.start()
    tell(hello_sem.at[0], at_z(zp))
    for k in (1, 2, 3):
        tell(hello_sem.at[1], (mod4(y + k), x, zh, c, zl))

    def rows_z(copies, local):
        for copy in copies:
            copy.wait_recv()
        local.wait()
        pl.semaphore_wait(hello_sem.at[0], 1)
        out = []
        for k in (2, 1, 3):
            zd = mod4(zh + k)
            cols = pl.ds(pl.multiple_of(zd * 128, 128), 128)
            out.append(send(rows1.at[:, :, cols], rows2.at[zh], at_z(zd)))
        local = pltpu.make_async_copy(
            rows1.at[:, :, pl.ds(pl.multiple_of(zh * 128, 128), 128)], rows2.at[zh], in_sem.at[1]
        )
        local.start()
        return out, local

    def rows_y(copies, local):
        for copy in copies:
            copy.wait_recv()
        local.wait()
        pl.semaphore_wait(hello_sem.at[1], 3)
        out = []
        for zd in range(4):
            own = jnp.logical_and(y == zl, zl == zd)
            remote = pltpu.make_async_remote_copy(
                src_ref=rows2, dst_ref=rows3.at[c, y], send_sem=out_send.at[zd],
                recv_sem=out_recv.at[y], device_id=(zl, x, zh, c, zd), device_id_type=MESH,
            )
            out.append((own, remote))

            @pl.when(own)
            def _():
                pltpu.make_async_copy(rows2, rows3.at[c, y], out_recv.at[y]).start()

            @pl.when(jnp.logical_not(own))
            def _():
                remote.start()

        return out

    def rows_core():
        for ys in range(4):
            pltpu.make_async_copy(rows2, rows3.at[c, ys], out_recv.at[ys]).wait()
        return send(rows3.at[c], rows3.at[c], partner)

    def block(z, sd, fd):
        return big.at[c, z, sd * d + fd * c, fd * d + sd * c]

    def half(z, sd, fd, k):
        return big.at[c, z, sd * d + fd * c, fd * d + sd * c, :, pl.ds(512 * k, 512)]

    slices = (zh, zm, zp, zo)
    F1, F2, S1, S2, X = {}, {}, {}, {}, {}

    def both_s(k, j, fd):
        z = slices[k]
        S1[k, j, 0] = send(block(z, s, fd), block(z, s, fd), at_s(sp))
        S1[k, j, 1] = send(block(z, s, fd), block(z, s, fd), at_s(sm))

    def stage_a(k):
        z = slices[k]
        F1[k, 0] = send(block(z, s, f), block(z, s, f), at_f(fp))
        F1[k, 1] = send(block(z, s, f), block(z, s, f), at_f(fm))
        both_s(k, 0, f)
        F2[k] = send(block(z, s, f), block(z, s, f), at_f(fo))

    def stage_b(k):
        F1[k, 0].wait_recv()
        both_s(k, 1, fm)
        F1[k, 1].wait_recv()
        both_s(k, 2, fp)

    def stage_c(k):
        z = slices[k]
        S1[k, 0, 0].wait_recv()
        S2[k, 0] = send(block(z, sm, f), block(z, sm, f), at_s(sp))

    def stage_d(k):
        F2[k].wait_recv()
        both_s(k, 3, fo)

    def stage_e(k):
        z = slices[k]
        S1[k, 1, 0].wait_recv()
        S2[k, 1] = send(block(z, sm, fm), block(z, sm, fm), at_s(sp))
        S1[k, 2, 1].wait_recv()
        S2[k, 2] = send(block(z, sp, fp), block(z, sp, fp), at_s(sm))

    def stage_f(k):
        z = slices[k]
        S1[k, 3, 1].wait_recv()
        S2[k, 3] = send(block(z, sp, fo), block(z, sp, fo), at_s(sm))

    def stage_g(k):
        z = slices[k]
        S1[k, 0, 1].wait_recv()
        S1[k, 1, 1].wait_recv()
        S1[k, 2, 0].wait_recv()
        S1[k, 3, 0].wait_recv()
        for j in range(4):
            S2[k, j].wait_recv()
        X[k] = send(big.at[c, z], big.at[c, z], partner)

    def finish_rows(last):
        last.wait_recv()
        row = lax.broadcasted_iota(jnp.int32, (256, 128), 0)
        lane = lax.broadcasted_iota(jnp.int32, (256, 128), 1)
        keep = lax.rem(row // 4, 2) == lane // 64
        straight = lane // 64 == c

        @pl.loop(0, 4)
        def _(z):
            parts = [rows3[core, :, z].reshape(16, 8, 128).astype(F32) for core in range(2)]
            data = jnp.stack(parts, axis=1).reshape(256, 128)
            turned = pltpu.roll(data, 64, 1)
            t = jnp.transpose(jnp.where(keep, jnp.where(straight, data, turned), 0.0))
            lhs_t[z] = t.astype(BF)
            lhs_sq[z] = (t * t).astype(BF)

    def dots(zs, j):
        cols = pl.ds(pl.multiple_of(lax.rem(j, 4) * TILE, TILE), TILE)
        rights = [big[j // 4, z, :, :, :, cols].reshape(256, TILE) for z in zs]
        right = jnp.concatenate(rights, axis=0)
        left = jnp.concatenate([lhs_t[z] for z in zs], axis=1)
        left_sq = jnp.concatenate([lhs_sq[z] for z in zs], axis=1)
        grad = jnp.dot(left, right, preferred_element_type=F32)
        square = jnp.dot(left_sq, sq_round(right), preferred_element_type=F32)
        return grad, square

    def mm_first(ks):
        for k in ks:
            X[k].wait_recv()

        @pl.loop(0, 8)
        def _(j):
            grad, square = dots([slices[k] for k in ks], j)
            wide = pl.ds(pl.multiple_of(j * TILE, TILE), TILE)
            acc_g[:, wide] = grad
            acc_s[:, wide] = square

    def mm_last():
        X[3].wait_recv()
        norm_acc[...] = jnp.zeros_like(norm_acc)

        @pl.loop(0, 8)
        def _(j):
            grad, square = dots([zo], j)
            wide = pl.ds(pl.multiple_of(j * TILE, TILE), TILE)
            grad = (acc_g[:, wide] + grad) / EXAMPLES
            base = (acc_s[:, wide] + square) / EXAMPLES + DAMPING
            precond = jnp.exp(EXPONENT * jnp.log(base))
            ratio = grad / precond
            p_all[:, wide] = precond
            r_all[:, wide] = ratio
            norm_acc[...] += jnp.sum(grad * ratio, axis=0, keepdims=True)

    exchange.wait_recv()
    first = c == 0
    mine = pair_src[c].astype(F32)
    other = pair_dst[...].astype(F32)
    low, high = jnp.where(first, mine, other), jnp.where(first, other, mine)
    big[c, zh, y, x] = jnp.concatenate([low, high], axis=0).astype(BF)

    z1a = send(half(zh, s, f, 0), half(zh, s, f, 0), at_z(zp))
    z1b = send(half(zh, s, f, 1), half(zh, s, f, 1), at_z(zm))
    stage_a(0)
    z1c = send(half(zh, s, f, 1), half(zh, s, f, 1), at_z(zp))
    z1d = send(half(zh, s, f, 0), half(zh, s, f, 0), at_z(zm))
    row_copies = rows_z(row_hop, row_own)
    stage_b(0)
    stage_c(0)
    z1a.wait_recv()
    z2p = send(half(zm, s, f, 0), half(zm, s, f, 0), at_z(zp))
    z1b.wait_recv()
    z2m = send(half(zp, s, f, 1), half(zp, s, f, 1), at_z(zm))
    stage_d(0)
    z1c.wait_recv()
    stage_a(1)
    z1d.wait_recv()
    stage_a(2)
    stage_e(0)
    stage_f(0)
    stage_b(1)
    stage_b(2)
    stage_c(1)
    stage_c(2)
    stage_d(1)
    stage_d(2)
    z2p.wait_recv()
    z2m.wait_recv()
    stage_a(3)
    row_copies = rows_y(*row_copies)
    stage_e(1)
    stage_e(2)
    stage_f(1)
    stage_f(2)
    stage_g(0)
    stage_b(3)
    stage_c(3)
    stage_d(3)
    stage_g(1)
    stage_g(2)
    stage_e(3)
    stage_f(3)
    last_rows = rows_core()
    stage_g(3)
    finish_rows(last_rows)
    mm_first((0, 1, 2))
    mm_last()

    own_norm = jnp.sum(norm_acc[...], axis=1, keepdims=True)
    plane = (y * 4 + x) * 2 + c
    red_a[plane] = jnp.broadcast_to(own_norm, (1, 128))

    @pl.loop(1, 32)
    def _(k):
        to = lax.rem(plane + k, 32)
        pltpu.make_async_remote_copy(
            src_ref=red_a.at[plane], dst_ref=red_a.at[plane], send_sem=red_send.at[0],
            recv_sem=red_recv.at[0],
            device_id=(to // 8, lax.rem(to // 2, 4), zh, lax.rem(to, 2), zl), device_id_type=MESH,
        ).start()

    pltpu.make_async_copy(red_a.at[pl.ds(0, 31)], red_a.at[pl.ds(0, 31)], red_recv.at[0]).wait()
    z16 = zh * 4 + zl
    red_b[z16] = jnp.sum(red_a[...], axis=0)

    @pl.loop(1, 16)
    def _(k):
        to = lax.rem(z16 + k, 16)
        pltpu.make_async_remote_copy(
            src_ref=red_b.at[z16], dst_ref=red_b.at[z16], send_sem=red_send.at[1],
            recv_sem=red_recv.at[1],
            device_id=(y, x, to // 4, c, lax.rem(to, 4)), device_id_type=MESH,
        ).start()

    for copy in sent:
        copy.wait_send()
    for own, remote in row_copies:

        @pl.when(jnp.logical_not(own))
        def _():
            remote.wait_send()

    pltpu.make_async_copy(red_a.at[pl.ds(0, 31)], red_a.at[pl.ds(0, 31)], red_send.at[0]).wait()
    pltpu.make_async_copy(red_b.at[pl.ds(0, 15)], red_b.at[pl.ds(0, 15)], red_recv.at[1]).wait()
    n_out[...] = jnp.sum(red_b[...], axis=0)
    pltpu.make_async_copy(red_b.at[pl.ds(0, 15)], red_b.at[pl.ds(0, 15)], red_send.at[1]).wait()


def scale_kernel(precond, ratio, norm, p_in, r_in, p_out, r_out, scaled, sem):
    copies = [
        pltpu.make_async_copy(precond.at[0:64], p_in, sem.at[0]),
        pltpu.make_async_copy(precond.at[64:128], p_out, sem.at[1]),
    ]
    for copy in copies:
        copy.start()
    rescale = jnp.sqrt(2.0 * D * H / norm[0:1, 0:1])
    for k, (target, rows) in enumerate(((r_in, 0), (r_in, 32), (r_out, 64), (r_out, 96))):
        scaled[rows : rows + 32] = ratio[rows : rows + 32] * rescale
        copy = pltpu.make_async_copy(
            scaled.at[rows : rows + 32], target.at[pl.ds(rows % 64, 32)], sem.at[2 + k]
        )
        copy.start()
        copies.append(copy)
    for copy in copies:
        copy.wait()


def shards(*args):
    hbm = pl.BlockSpec(memory_space=pltpu.HBM)
    vmem = pl.BlockSpec(memory_space=pltpu.VMEM)
    dma = pltpu.SemaphoreType.DMA
    both = pltpu.VMEM((128, 2048), F32)
    precond, ratio, norm = pl.pallas_call(
        kernel,
        out_shape=(both, both, pltpu.VMEM((1, 128), F32)),
        in_specs=[hbm] * 4,
        out_specs=(vmem,) * 3,
        scratch_shapes=[
            pltpu.VMEM((4, 2048), BF),
            pltpu.VMEM((4, 2048), BF),
            pltpu.VMEM((4, 2048), BF),
            pltpu.VMEM((4, 2048), BF),
            pltpu.VMEM((2, 8, 2048), F32),
            pltpu.VMEM((4, 8, 512), BF),
            pltpu.VMEM((2, 8, 1024), BF),
            pltpu.VMEM((8, 1024), BF),
            pltpu.VMEM((2, 4, 4, 4, 16, 1024), BF),
            pltpu.VMEM((4, 8, 512), BF),
            pltpu.VMEM((4, 4, 8, 128), BF),
            pltpu.VMEM((2, 4, 4, 4, 8, 128), BF),
            pltpu.VMEM((4, 128, 256), BF),
            pltpu.VMEM((4, 128, 256), BF),
            pltpu.VMEM((128, 2048), F32),
            pltpu.VMEM((128, 2048), F32),
            pltpu.VMEM((1, TILE), F32),
            pltpu.VMEM((32, 1, 128), F32),
            pltpu.VMEM((16, 1, 128), F32),
            dma((4,)),
            dma((N_MSG,)),
            dma((N_MSG,)),
            dma((4,)),
            dma((4,)),
            dma((2,)),
            dma((2,)),
            pltpu.SemaphoreType.REGULAR((2,)),
        ],
        compiler_params=pltpu.CompilerParams(
            collective_id=0, has_side_effects=True, vmem_limit_bytes=K1_LIMIT
        ),
    )(*(pltpu.with_memory_space_constraint(v, pltpu.HBM) for v in args))
    half = jax.ShapeDtypeStruct((64, 2048), F32)
    outs = pl.pallas_call(
        scale_kernel,
        out_shape=(half,) * 4,
        in_specs=[vmem] * 3,
        out_specs=(hbm,) * 4,
        scratch_shapes=[pltpu.VMEM((128, 2048), F32), dma((6,))],
        compiler_params=pltpu.CompilerParams(vmem_limit_bytes=8 * 1024 * 1024),
    )(*(pltpu.with_memory_space_constraint(v, pltpu.VMEM) for v in (precond, ratio, norm)))
    return (*outs, norm[0, 0])


def solution(mesh):
    torus = Mesh(mesh.devices.reshape(4, 4, 4, 2, mesh.shape["mp"]), AXES)
    placed = (P(DP, None), P(DP, "mp"), P(DP, "mp"), P(DP, "mp"))
    return jax.shard_map(
        shards,
        mesh=torus,
        in_specs=placed,
        out_specs=(P(DP, "mp"), P(DP, "mp"), P(DP, "mp"), P(DP, "mp"), P()),
        check_vma=False,
    )
```

```python
import jax
import jax.numpy as jnp
from jax import lax
from jax.experimental import pallas as pl
from jax.experimental.pallas import tpu as pltpu
from jax.sharding import Mesh
from jax.sharding import PartitionSpec as P

D = 8192
H = 8192
EXAMPLES = 512
DP = ("dp_0", "dp_1", "dp_2", "dp_3")
AXES = ("dp_0", "dp_1", "dp_2", "dp_3", "mp")
MESH = pl.DeviceIdType.MESH
BF = jnp.bfloat16
F32 = jnp.float32

DAMPING = 0.1
EXPONENT = 0.75

SMALL, GATHER, FORWARD, RED_A, RED_B = range(5)
N_LANDED = 52
TILE = 256
K1_LIMIT = 32 * 1024 * 1024


def mod4(a):
    return lax.rem(a, 4)


def kernel(
    li_hbm, pre_hbm, ha_hbm, oa_hbm,
    p_all, r_all, n_out,
    pre_v, ha_v, oa_v, li_v, stack, rows0, pair_src,
    big, rows1, rows2, rows3, lhs_t, lhs_sq, acc_g, acc_s, norm_acc, red_a, red_b,
    in_sem, left, landed, out_sem, hello_sem,
):
    y, x, zh, c, zl = (lax.axis_index(a) for a in AXES)
    d = 1 - c
    f = x * d + y * c
    s = y * d + x * c
    fp, fm, fo = mod4(f + 1), mod4(f + 3), mod4(f + 2)
    sp, sm, so = mod4(s + 1), mod4(s + 3), mod4(s + 2)
    zp, zm, zo = mod4(zh + 1), mod4(zh + 3), mod4(zh + 2)

    def at_f(fd):
        return (y * d + fd * c, fd * d + x * c, zh, c, zl)

    def at_s(sd):
        return (sd * d + y * c, x * d + sd * c, zh, c, zl)

    def at_z(zd, core=None):
        return (y, x, zd, c if core is None else core, zl)

    partner = (y, x, zh, d, zl)

    barrier = pltpu.get_barrier_semaphore()

    def tell(semaphore, device):
        pl.semaphore_signal(semaphore, inc=1, device_id=device, device_id_type=MESH)

    for core in (c, d):
        tell(barrier, at_z(zp, core))
        tell(barrier, at_z(zm, core))
    for k in (1, 2, 3):
        tell(barrier, (y, x, zh, c, mod4(zl + k)))
        tell(barrier, (mod4(y + k), x, zh, c, zl))
        tell(barrier, (y, mod4(x + k), zh, c, zl))
    tell(barrier, partner)

    loads = [
        pltpu.make_async_copy(pre_hbm, pre_v, in_sem.at[0]),
        pltpu.make_async_copy(ha_hbm, ha_v, in_sem.at[1]),
        pltpu.make_async_copy(oa_hbm, oa_v, in_sem.at[2]),
        pltpu.make_async_copy(
            li_hbm.at[:, pl.ds(pl.multiple_of(zl * 2048, 2048), 2048)], li_v, in_sem.at[3]
        ),
    ]
    for load in loads:
        load.start()
    for load in loads:
        load.wait()
    preact = pre_v[...].astype(F32)
    logistic = 1.0 / (1.0 + jnp.exp(-preact))
    hidden = (preact * logistic).astype(BF)
    adjoint = (ha_v[...].astype(F32) * logistic * (1.0 + preact * (1.0 - logistic))).astype(BF)
    stack[0, 0:4, :] = adjoint.astype(F32)
    stack[0, 4:8, :] = oa_v[...].astype(F32)
    stack[1, 0:4, :] = li_v[...].astype(F32)
    stack[1, 4:8, :] = hidden.astype(F32)
    pair_src[0] = stack[0, :, 0:1024].astype(BF)
    pair_src[1] = stack[0, :, 1024:2048].astype(BF)
    big[c, zh, y, x, c] = pair_src[c]
    for k in range(4):
        rows0[k] = stack[1, :, 512 * k : 512 * (k + 1)].astype(BF)

    pl.semaphore_wait(barrier, 14)

    places = {}

    def place(key):
        return landed.at[places.setdefault(key, len(places))]

    def send(src, dst, device, key, group):
        pltpu.make_async_remote_copy(
            src_ref=src, dst_ref=dst, send_sem=left.at[group], recv_sem=place(key),
            device_id=device, device_id_type=MESH,
        ).start()

    def take(ref, semaphore):
        pltpu.make_async_copy(ref, ref, semaphore).wait()

    def arrived(ref, key):
        take(ref, place(key))

    one = big.at[0, 0, 0, 0]
    half_block = big.at[0, 0, 0, 0, :, :, 0:512]

    def block(z, sd, fd):
        return big.at[c, z, sd * d + fd * c, fd * d + sd * c]

    def half(z, sd, fd, k):
        return big.at[c, z, sd * d + fd * c, fd * d + sd * c, :, :, pl.ds(512 * k, 512)]

    def z_pieces(zd, k, key):
        cols = pl.ds(512 * k, 512)
        for core in (c, d):
            send(
                pair_src.at[core, :, cols], big.at[core, zh, y, x, c, :, cols],
                at_z(zd, core), key, SMALL,
            )

    z_pieces(zp, 0, "z1a")
    z_pieces(zm, 1, "z1b")
    send(pair_src.at[d], big.at[d, zh, y, x, c], partner, "pair", SMALL)
    for k in (1, 2, 3):
        xd = mod4(x + k)
        send(rows0.at[xd], rows1.at[x], (y, xd, zh, c, zl), "row_x", SMALL)
    row_own = pltpu.make_async_copy(rows0.at[x], rows1.at[x], in_sem.at[0])
    row_own.start()
    z_pieces(zp, 1, "z1c")
    z_pieces(zm, 0, "z1d")
    tell(hello_sem.at[0], at_z(zp))
    for k in (1, 2, 3):
        tell(hello_sem.at[1], (mod4(y + k), x, zh, c, zl))

    def rows_z():
        arrived(rows1.at[0:3], "row_x")
        row_own.wait()
        pl.semaphore_wait(hello_sem.at[0], 1)
        for zd, key in ((zo, "row_z_far"), (zp, "row_z"), (zm, "row_z")):
            cols = pl.ds(pl.multiple_of(zd * 128, 128), 128)
            send(rows1.at[:, :, cols], rows2.at[zh], at_z(zd), key, SMALL)
        local = pltpu.make_async_copy(
            rows1.at[:, :, pl.ds(pl.multiple_of(zh * 128, 128), 128)], rows2.at[zh], in_sem.at[1]
        )
        local.start()
        return local

    def rows_y(planes, key):
        for zd in range(4):
            own = jnp.logical_and(y == zl, zl == zd)
            for z in planes:

                @pl.when(own)
                def _():
                    pltpu.make_async_copy(rows2.at[z], rows3.at[c, z, y], place(key)).start()

                @pl.when(jnp.logical_not(own))
                def _():
                    pltpu.make_async_remote_copy(
                        src_ref=rows2.at[z], dst_ref=rows3.at[c, z, y], send_sem=out_sem.at[zd],
                        recv_sem=place(key), device_id=(zl, x, zh, c, zd), device_id_type=MESH,
                    ).start()

    def rows_near(local):
        arrived(rows2.at[0:2], "row_z")
        local.wait()
        pl.semaphore_wait(hello_sem.at[1], 3)
        rows_y((zh, zm, zp), "row_y")

    def rows_far():
        arrived(rows2.at[0], "row_z_far")
        rows_y((zo,), "row_y_far")

    def rows_core_near():
        arrived(rows3.at[0, 0:3], "row_y")
        for z in (zh, zm, zp):
            send(rows3.at[c, z], rows3.at[c, z], partner, "row_core", SMALL)

    def rows_core_far():
        arrived(rows3.at[0, 0], "row_y_far")
        send(rows3.at[c, zo], rows3.at[c, zo], partner, "row_core_far", SMALL)

    slices = (zh, zm, zp, zo)
    routes = {0: "++--", 1: "++--", 2: "++--", 3: "-+-*"}

    def s_key(k, j, side):
        relayed = {"+": 0, "-": 1}.get(routes[k][j])
        if relayed == side:
            return ("s1", k, j)
        return ("rest", k, 0)

    def far_key(k):
        return ("rest", k, 1 if k == 3 else 0)

    def both_s(k, j, fd):
        z = slices[k]
        send(block(z, s, fd), block(z, s, fd), at_s(sp), s_key(k, j, 0), GATHER)
        send(block(z, s, fd), block(z, s, fd), at_s(sm), s_key(k, j, 1), GATHER)
        if routes[k][j] == "*":
            send(block(z, s, fd), block(z, s, fd), at_s(so), far_key(k), GATHER)

    def relay(k, j, fd):
        z = slices[k]
        arrived(one, ("s1", k, j))
        came, goes = (sm, sp) if routes[k][j] == "+" else (sp, sm)
        send(block(z, came, fd), block(z, came, fd), at_s(goes), far_key(k), GATHER)

    def stage_a(k):
        z = slices[k]
        send(block(z, s, f), block(z, s, f), at_f(fp), ("f1", k, 0), GATHER)
        send(block(z, s, f), block(z, s, f), at_f(fm), ("f1", k, 1), GATHER)
        both_s(k, 0, f)
        send(block(z, s, f), block(z, s, f), at_f(fo), ("f2", k), GATHER)

    def stage_b(k):
        arrived(one, ("f1", k, 0))
        both_s(k, 1, fm)
        arrived(one, ("f1", k, 1))
        both_s(k, 2, fp)

    def stage_c(k):
        relay(k, 0, f)

    def stage_d(k):
        arrived(one, ("f2", k))
        both_s(k, 3, fo)

    def stage_e(k):
        relay(k, 1, fm)
        relay(k, 2, fp)

    def stage_f(k):
        relay(k, 3, fo)

    def stage_g(k):
        z = slices[k]
        arrived(big.at[0, 0, 0:2], ("rest", k, 0))
        send(big.at[c, z], big.at[c, z], partner, ("x", k), FORWARD)

    def forward(z, sd):
        for fd in (f, fm, fp, fo):
            send(block(z, sd, fd), block(z, sd, fd), partner, ("x", 3), FORWARD)

    def last_near():
        arrived(big.at[0, 0, 0:2, :, :, :, 0:640], ("rest", 3, 0))
        forward(zo, sm)
        forward(zo, sp)

    def last_far():
        arrived(big.at[0, 0, 0], ("rest", 3, 1))
        forward(zo, so)

    def finish_rows(z):
        row = lax.broadcasted_iota(jnp.int32, (256, 128), 0)
        lane = lax.broadcasted_iota(jnp.int32, (256, 128), 1)
        keep = lax.rem(row // 4, 2) == lane // 64
        straight = lane // 64 == c
        parts = [rows3[core, z].reshape(16, 8, 128).astype(F32) for core in range(2)]
        data = jnp.stack(parts, axis=1).reshape(256, 128)
        turned = pltpu.roll(data, 64, 1)
        t = jnp.transpose(jnp.where(keep, jnp.where(straight, data, turned), 0.0))
        lhs_t[z] = t.astype(BF)
        lhs_sq[z] = (t * t).astype(BF)

    def finish_near():
        arrived(rows3.at[0, 0:3], "row_core")

        @pl.loop(0, 3)
        def _(k):
            finish_rows(mod4(zh + k + 3))

    def finish_far():
        arrived(rows3.at[0, 0], "row_core_far")
        finish_rows(zo)

    def dots(zs, j):
        cols = pl.ds(pl.multiple_of(lax.rem(j, 4) * TILE, TILE), TILE)
        rights = [big[j // 4, z, :, :, :, :, cols].astype(F32).reshape(256, TILE) for z in zs]
        right = jnp.concatenate(rights, axis=0)
        left_t = jnp.concatenate([lhs_t[z] for z in zs], axis=1)
        left_sq = jnp.concatenate([lhs_sq[z] for z in zs], axis=1)
        grad = jnp.dot(left_t, right.astype(BF), preferred_element_type=F32)
        square = jnp.dot(left_sq, (right * right).astype(BF), preferred_element_type=F32)
        return grad, square

    def mm_part(ks, first):
        for k in ks:
            arrived(big.at[0, 0], ("x", k))

        @pl.loop(0, 8, unroll=8)
        def _(j):
            grad, square = dots([slices[k] for k in ks], j)
            wide = pl.ds(pl.multiple_of(j * TILE, TILE), TILE)
            if first:
                acc_g[:, wide] = grad
                acc_s[:, wide] = square
            else:
                acc_g[:, wide] += grad
                acc_s[:, wide] += square

    def mm_last():
        arrived(big.at[0, 0], ("x", 3))
        norm_acc[...] = jnp.zeros_like(norm_acc)

        @pl.loop(0, 8, unroll=8)
        def _(j):
            grad, square = dots([zo], j)
            wide = pl.ds(pl.multiple_of(j * TILE, TILE), TILE)
            grad = (acc_g[:, wide] + grad) * (1.0 / EXAMPLES)
            base = (acc_s[:, wide] + square) * (1.0 / EXAMPLES) + DAMPING
            power = EXPONENT * jnp.log(base)
            ratio = grad * jnp.exp(-power)
            p_all[:, wide] = jnp.exp(power)
            r_all[:, wide] = ratio
            norm_acc[...] += jnp.sum((grad * ratio).reshape(16, 8, TILE), axis=0)

    arrived(big.at[0, 0, 0, 0, 0], "pair")
    stage_a(0)
    stage_b(0)
    stage_c(0)
    rows_own = rows_z()
    stage_d(0)
    arrived(half_block, "z1a")
    send(half(zm, s, f, 0), half(zm, s, f, 0), at_z(zp), "z2p", SMALL)
    arrived(half_block, "z1b")
    send(half(zp, s, f, 1), half(zp, s, f, 1), at_z(zm), "z2m", SMALL)
    arrived(half_block, "z1c")
    stage_a(1)
    arrived(half_block, "z1d")
    stage_a(2)
    stage_e(0)
    stage_f(0)
    stage_b(1)
    stage_b(2)
    stage_c(1)
    stage_c(2)
    stage_d(1)
    stage_d(2)
    rows_near(rows_own)
    arrived(half_block, "z2p")
    arrived(half_block, "z2m")
    stage_a(3)
    stage_e(1)
    stage_e(2)
    stage_g(0)
    stage_f(1)
    stage_f(2)
    stage_b(3)
    stage_c(3)
    rows_far()
    stage_d(3)
    rows_core_near()
    stage_g(1)
    stage_g(2)
    stage_e(3)
    forward(zo, s)
    rows_core_far()
    finish_near()
    mm_part((0, 1, 2), True)
    last_near()
    last_far()
    finish_far()
    mm_last()

    own_norm = jnp.sum(jnp.sum(norm_acc[...], axis=1, keepdims=True), axis=0, keepdims=True)
    plane = (y * 4 + x) * 2 + c
    red_a[plane] = jnp.broadcast_to(own_norm, (1, 128))

    @pl.loop(0, 31)
    def _(k):
        to = lax.rem(plane + 1 + lax.rem(k + 16, 31), 32)
        send(
            red_a.at[plane], red_a.at[plane],
            (to // 8, lax.rem(to // 2, 4), zh, lax.rem(to, 2), zl), "red_a", RED_A,
        )

    arrived(red_a.at[0:31], "red_a")
    z16 = zh * 4 + zl
    red_b[z16] = jnp.sum(red_a[...], axis=0)

    @pl.loop(0, 15)
    def _(k):
        to = lax.rem(z16 + 1 + lax.rem(k + 7, 15), 16)
        send(
            red_b.at[z16], red_b.at[z16], (y, x, to // 4, c, lax.rem(to, 4)), "red_b", RED_B
        )

    take(big.at[:, 0:3, 0:3, 0, 0], left.at[SMALL])
    take(big.at[:, 0:3, :, :, :, :, 0:640], left.at[GATHER])
    take(big.at[0], left.at[FORWARD])
    for zd in range(4):

        @pl.when(jnp.logical_not(jnp.logical_and(y == zl, zl == zd)))
        def _():
            take(rows2, out_sem.at[zd])

    take(red_a.at[0:31], left.at[RED_A])
    arrived(red_b.at[0:15], "red_b")
    n_out[...] = jnp.sum(red_b[...], axis=0)
    take(red_b.at[0:15], left.at[RED_B])
    assert len(places) == N_LANDED, len(places)


def scale_kernel(precond, ratio, norm, p_in, r_in, p_out, r_out, scaled, sem):
    copies = [
        pltpu.make_async_copy(precond.at[0:64], p_in, sem.at[0]),
        pltpu.make_async_copy(precond.at[64:128], p_out, sem.at[1]),
    ]
    for copy in copies:
        copy.start()
    rescale = jnp.sqrt(2.0 * D * H / norm[0:1, 0:1])
    for k, (target, rows) in enumerate(((r_in, 0), (r_in, 32), (r_out, 64), (r_out, 96))):
        scaled[rows : rows + 32] = ratio[rows : rows + 32] * rescale
        copy = pltpu.make_async_copy(
            scaled.at[rows : rows + 32], target.at[pl.ds(rows % 64, 32)], sem.at[2 + k]
        )
        copy.start()
        copies.append(copy)
    for copy in copies:
        copy.wait()


def shards(*args):
    hbm = pl.BlockSpec(memory_space=pltpu.HBM)
    vmem = pl.BlockSpec(memory_space=pltpu.VMEM)
    dma = pltpu.SemaphoreType.DMA
    both = pltpu.VMEM((128, 2048), F32)
    precond, ratio, norm = pl.pallas_call(
        kernel,
        out_shape=(both, both, pltpu.VMEM((1, 128), F32)),
        in_specs=[hbm] * 4,
        out_specs=(vmem,) * 3,
        scratch_shapes=[
            pltpu.VMEM((4, 2048), BF),
            pltpu.VMEM((4, 2048), BF),
            pltpu.VMEM((4, 2048), BF),
            pltpu.VMEM((4, 2048), BF),
            pltpu.VMEM((2, 8, 2048), F32),
            pltpu.VMEM((4, 8, 512), BF),
            pltpu.VMEM((2, 8, 1024), BF),
            pltpu.VMEM((2, 4, 4, 4, 2, 8, 1024), BF),
            pltpu.VMEM((4, 8, 512), BF),
            pltpu.VMEM((4, 4, 8, 128), BF),
            pltpu.VMEM((2, 4, 4, 4, 8, 128), BF),
            pltpu.VMEM((4, 128, 256), BF),
            pltpu.VMEM((4, 128, 256), BF),
            pltpu.VMEM((128, 2048), F32),
            pltpu.VMEM((128, 2048), F32),
            pltpu.VMEM((8, TILE), F32),
            pltpu.VMEM((32, 1, 128), F32),
            pltpu.VMEM((16, 1, 128), F32),
            dma((4,)),
            dma((5,)),
            dma((N_LANDED,)),
            dma((4,)),
            pltpu.SemaphoreType.REGULAR((2,)),
        ],
        compiler_params=pltpu.CompilerParams(
            collective_id=0, has_side_effects=True, vmem_limit_bytes=K1_LIMIT
        ),
    )(*(pltpu.with_memory_space_constraint(v, pltpu.HBM) for v in args))
    half = jax.ShapeDtypeStruct((64, 2048), F32)
    outs = pl.pallas_call(
        scale_kernel,
        out_shape=(half,) * 4,
        in_specs=[vmem] * 3,
        out_specs=(hbm,) * 4,
        scratch_shapes=[pltpu.VMEM((128, 2048), F32), dma((6,))],
        compiler_params=pltpu.CompilerParams(vmem_limit_bytes=8 * 1024 * 1024),
    )(*(pltpu.with_memory_space_constraint(v, pltpu.VMEM) for v in (precond, ratio, norm)))
    return (*outs, norm[0, 0])


def solution(mesh):
    torus = Mesh(mesh.devices.reshape(4, 4, 4, 2, mesh.shape["mp"]), AXES)
    placed = (P(DP, None), P(DP, "mp"), P(DP, "mp"), P(DP, "mp"))
    return jax.shard_map(
        shards,
        mesh=torus,
        in_specs=placed,
        out_specs=(P(DP, "mp"), P(DP, "mp"), P(DP, "mp"), P(DP, "mp"), P()),
        check_vma=False,
    )
```

```python
import jax
import jax.numpy as jnp
from jax import lax
from jax.experimental import pallas as pl
from jax.experimental.pallas import tpu as pltpu
from jax.sharding import Mesh
from jax.sharding import PartitionSpec as P

D = 8192
H = 8192
EXAMPLES = 512
DP = ("dp_0", "dp_1", "dp_2", "dp_3")
AXES = ("dp_0", "dp_1", "dp_2", "dp_3", "mp")
MESH = pl.DeviceIdType.MESH
BF = jnp.bfloat16
F32 = jnp.float32

DAMPING = 0.1
EXPONENT = 0.75

SMALL, GATHER, FORWARD, RED_A, RED_B = range(5)
N_LANDED = 52
TILE = 256
K1_LIMIT = 32 * 1024 * 1024


def mod4(a):
    return lax.rem(a, 4)


def kernel(
    li_hbm, pre_hbm, ha_hbm, oa_hbm,
    p_all, r_all, n_out,
    pre_v, ha_v, oa_v, li_v, stack, rows0, pair_src,
    big, rows1, rows2, rows3, lhs_t, lhs_sq, acc_g, acc_s, norm_acc, red_a, red_b,
    in_sem, left, landed, out_sem, hello_sem,
):
    y, x, zh, c, zl = (lax.axis_index(a) for a in AXES)
    d = 1 - c
    f = x * d + y * c
    s = y * d + x * c
    fp, fm, fo = mod4(f + 1), mod4(f + 3), mod4(f + 2)
    sp, sm, so = mod4(s + 1), mod4(s + 3), mod4(s + 2)
    zp, zm, zo = mod4(zh + 1), mod4(zh + 3), mod4(zh + 2)

    def at_f(fd):
        return (y * d + fd * c, fd * d + x * c, zh, c, zl)

    def at_s(sd):
        return (sd * d + y * c, x * d + sd * c, zh, c, zl)

    def at_z(zd, core=None):
        return (y, x, zd, c if core is None else core, zl)

    partner = (y, x, zh, d, zl)

    barrier = pltpu.get_barrier_semaphore()

    def tell(semaphore, device):
        pl.semaphore_signal(semaphore, inc=1, device_id=device, device_id_type=MESH)

    for core in (c, d):
        tell(barrier, at_z(zp, core))
        tell(barrier, at_z(zm, core))
    for k in (1, 2, 3):
        tell(barrier, (y, x, zh, c, mod4(zl + k)))
        tell(barrier, (mod4(y + k), x, zh, c, zl))
        tell(barrier, (y, mod4(x + k), zh, c, zl))
    tell(barrier, partner)

    loads = [
        pltpu.make_async_copy(pre_hbm, pre_v, in_sem.at[0]),
        pltpu.make_async_copy(ha_hbm, ha_v, in_sem.at[1]),
        pltpu.make_async_copy(oa_hbm, oa_v, in_sem.at[2]),
        pltpu.make_async_copy(
            li_hbm.at[:, pl.ds(pl.multiple_of(zl * 2048, 2048), 2048)], li_v, in_sem.at[3]
        ),
    ]
    for load in loads:
        load.start()
    for load in loads:
        load.wait()
    preact = pre_v[...].astype(F32)
    logistic = 1.0 / (1.0 + jnp.exp(-preact))
    hidden = (preact * logistic).astype(BF)
    adjoint = (ha_v[...].astype(F32) * logistic * (1.0 + preact * (1.0 - logistic))).astype(BF)
    stack[0, 0:4, :] = adjoint.astype(F32)
    stack[0, 4:8, :] = oa_v[...].astype(F32)
    stack[1, 0:4, :] = li_v[...].astype(F32)
    stack[1, 4:8, :] = hidden.astype(F32)
    pair_src[0] = stack[0, :, 0:1024].astype(BF)
    pair_src[1] = stack[0, :, 1024:2048].astype(BF)
    big[c, zh, y, x, c] = pair_src[c]
    for k in range(4):
        rows0[k] = stack[1, :, 512 * k : 512 * (k + 1)].astype(BF)

    pl.semaphore_wait(barrier, 14)

    places = {}

    def place(key):
        return landed.at[places.setdefault(key, len(places))]

    def send(src, dst, device, key, group):
        pltpu.make_async_remote_copy(
            src_ref=src, dst_ref=dst, send_sem=left.at[group], recv_sem=place(key),
            device_id=device, device_id_type=MESH,
        ).start()

    def take(ref, semaphore):
        pltpu.make_async_copy(ref, ref, semaphore).wait()

    def arrived(ref, key):
        take(ref, place(key))

    one = big.at[0, 0, 0, 0]
    half_block = big.at[0, 0, 0, 0, :, :, 0:512]

    def block(z, sd, fd):
        return big.at[c, z, sd * d + fd * c, fd * d + sd * c]

    def half(z, sd, fd, k):
        return big.at[c, z, sd * d + fd * c, fd * d + sd * c, :, :, pl.ds(512 * k, 512)]

    def z_pieces(zd, k, key):
        cols = pl.ds(512 * k, 512)
        for core in (c, d):
            send(
                pair_src.at[core, :, cols], big.at[core, zh, y, x, c, :, cols],
                at_z(zd, core), key, SMALL,
            )

    z_pieces(zp, 0, "z1a")
    z_pieces(zm, 1, "z1b")
    send(pair_src.at[d], big.at[d, zh, y, x, c], partner, "pair", SMALL)
    for k in (1, 2, 3):
        xd = mod4(x + k)
        send(rows0.at[xd], rows1.at[x], (y, xd, zh, c, zl), "row_x", SMALL)
    row_own = pltpu.make_async_copy(rows0.at[x], rows1.at[x], in_sem.at[0])
    row_own.start()
    z_pieces(zp, 1, "z1c")
    z_pieces(zm, 0, "z1d")
    tell(hello_sem.at[0], at_z(zp))
    for k in (1, 2, 3):
        tell(hello_sem.at[1], (mod4(y + k), x, zh, c, zl))

    def rows_z():
        arrived(rows1.at[0:3], "row_x")
        row_own.wait()
        pl.semaphore_wait(hello_sem.at[0], 1)
        for zd, key in ((zo, "row_z_far"), (zp, "row_z"), (zm, "row_z")):
            cols = pl.ds(pl.multiple_of(zd * 128, 128), 128)
            send(rows1.at[:, :, cols], rows2.at[zh], at_z(zd), key, SMALL)
        local = pltpu.make_async_copy(
            rows1.at[:, :, pl.ds(pl.multiple_of(zh * 128, 128), 128)], rows2.at[zh], in_sem.at[1]
        )
        local.start()
        return local

    def rows_y(planes, key):
        for zd in range(4):
            own = jnp.logical_and(y == zl, zl == zd)
            for z in planes:

                @pl.when(own)
                def _():
                    pltpu.make_async_copy(rows2.at[z], rows3.at[c, z, y], place(key)).start()

                @pl.when(jnp.logical_not(own))
                def _():
                    pltpu.make_async_remote_copy(
                        src_ref=rows2.at[z], dst_ref=rows3.at[c, z, y], send_sem=out_sem.at[zd],
                        recv_sem=place(key), device_id=(zl, x, zh, c, zd), device_id_type=MESH,
                    ).start()

    def rows_near(local):
        arrived(rows2.at[0:2], "row_z")
        local.wait()
        pl.semaphore_wait(hello_sem.at[1], 3)
        rows_y((zh, zm, zp), "row_y")

    def rows_far():
        arrived(rows2.at[0], "row_z_far")
        rows_y((zo,), "row_y_far")

    def rows_core_near():
        arrived(rows3.at[0, 0:3], "row_y")
        for z in (zh, zm, zp):
            send(rows3.at[c, z], rows3.at[c, z], partner, "row_core", SMALL)

    def rows_core_far():
        arrived(rows3.at[0, 0], "row_y_far")
        send(rows3.at[c, zo], rows3.at[c, zo], partner, "row_core_far", SMALL)

    slices = (zh, zm, zp, zo)
    routes = {0: "++--", 1: "++--", 2: "++--", 3: "-+-*"}

    def s_key(k, j, side):
        relayed = {"+": 0, "-": 1}.get(routes[k][j])
        if relayed == side:
            return ("s1", k, j)
        return ("rest", k, 0)

    def far_key(k):
        return ("rest", k, 1 if k == 3 else 0)

    def forward(k, sd, fd):
        z = slices[k]
        send(block(z, sd, fd), block(z, sd, fd), partner, ("x", k), FORWARD)

    def both_s(k, j, fd):
        z = slices[k]
        send(block(z, s, fd), block(z, s, fd), at_s(sp), s_key(k, j, 0), GATHER)
        send(block(z, s, fd), block(z, s, fd), at_s(sm), s_key(k, j, 1), GATHER)
        if routes[k][j] == "*":
            send(block(z, s, fd), block(z, s, fd), at_s(so), far_key(k), GATHER)
        forward(k, s, fd)

    def relay(k, j, fd):
        z = slices[k]
        arrived(one, ("s1", k, j))
        came, goes = (sm, sp) if routes[k][j] == "+" else (sp, sm)
        send(block(z, came, fd), block(z, came, fd), at_s(goes), far_key(k), GATHER)
        forward(k, came, fd)

    def stage_a(k):
        z = slices[k]
        send(block(z, s, f), block(z, s, f), at_f(fp), ("f1", k, 0), GATHER)
        send(block(z, s, f), block(z, s, f), at_f(fm), ("f1", k, 1), GATHER)
        both_s(k, 0, f)
        send(block(z, s, f), block(z, s, f), at_f(fo), ("f2", k), GATHER)

    def stage_b(k):
        arrived(one, ("f1", k, 0))
        both_s(k, 1, fm)
        arrived(one, ("f1", k, 1))
        both_s(k, 2, fp)

    def stage_c(k):
        relay(k, 0, f)

    def stage_d(k):
        arrived(one, ("f2", k))
        both_s(k, 3, fo)

    def stage_e(k):
        relay(k, 1, fm)
        relay(k, 2, fp)

    def stage_f(k):
        relay(k, 3, fo)

    def forward_near(k):
        for j, fd in enumerate((f, fm, fp, fo)):
            if routes[k][j] != "+":
                forward(k, sm, fd)
            if routes[k][j] != "-":
                forward(k, sp, fd)

    def stage_g(k):
        arrived(big.at[0, 0, 0:2], ("rest", k, 0))
        forward_near(k)
        for fd in (f, fm, fp, fo):
            forward(k, so, fd)

    def last_near():
        arrived(big.at[0, 0, 0:2, :, :, :, 0:640], ("rest", 3, 0))
        forward_near(3)

    def last_far():
        arrived(big.at[0, 0, 0], ("rest", 3, 1))
        for fd in (f, fm, fp, fo):
            forward(3, so, fd)

    def finish_rows(z):
        row = lax.broadcasted_iota(jnp.int32, (256, 128), 0)
        lane = lax.broadcasted_iota(jnp.int32, (256, 128), 1)
        keep = lax.rem(row // 4, 2) == lane // 64
        straight = lane // 64 == c
        parts = [rows3[core, z].reshape(16, 8, 128).astype(F32) for core in range(2)]
        data = jnp.stack(parts, axis=1).reshape(256, 128)
        turned = pltpu.roll(data, 64, 1)
        t = jnp.transpose(jnp.where(keep, jnp.where(straight, data, turned), 0.0))
        lhs_t[z] = t.astype(BF)
        lhs_sq[z] = (t * t).astype(BF)

    def finish_near():
        arrived(rows3.at[0, 0:3], "row_core")

        @pl.loop(0, 3)
        def _(k):
            finish_rows(mod4(zh + k + 3))

    def finish_far():
        arrived(rows3.at[0, 0], "row_core_far")
        finish_rows(zo)

    def dots(zs, j):
        cols = pl.ds(pl.multiple_of(lax.rem(j, 4) * TILE, TILE), TILE)
        rights = [big[j // 4, z, :, :, :, :, cols].astype(F32).reshape(256, TILE) for z in zs]
        right = jnp.concatenate(rights, axis=0)
        left_t = jnp.concatenate([lhs_t[z] for z in zs], axis=1)
        left_sq = jnp.concatenate([lhs_sq[z] for z in zs], axis=1)
        grad = jnp.dot(left_t, right.astype(BF), preferred_element_type=F32)
        square = jnp.dot(left_sq, (right * right).astype(BF), preferred_element_type=F32)
        return grad, square

    def mm_part(ks, first):
        for k in ks:
            arrived(big.at[0, 0], ("x", k))

        @pl.loop(0, 8, unroll=8)
        def _(j):
            grad, square = dots([slices[k] for k in ks], j)
            wide = pl.ds(pl.multiple_of(j * TILE, TILE), TILE)
            if first:
                acc_g[:, wide] = grad
                acc_s[:, wide] = square
            else:
                acc_g[:, wide] += grad
                acc_s[:, wide] += square

    def mm_last():
        arrived(big.at[0, 0], ("x", 3))
        norm_acc[...] = jnp.zeros_like(norm_acc)

        @pl.loop(0, 8, unroll=8)
        def _(j):
            grad, square = dots([zo], j)
            wide = pl.ds(pl.multiple_of(j * TILE, TILE), TILE)
            grad = (acc_g[:, wide] + grad) * (1.0 / EXAMPLES)
            base = (acc_s[:, wide] + square) * (1.0 / EXAMPLES) + DAMPING
            power = EXPONENT * jnp.log(base)
            ratio = grad * jnp.exp(-power)
            p_all[:, wide] = jnp.exp(power)
            r_all[:, wide] = ratio
            norm_acc[...] += jnp.sum((grad * ratio).reshape(16, 8, TILE), axis=0)

    arrived(big.at[0, 0, 0, 0, 0], "pair")
    stage_a(0)
    stage_b(0)
    stage_c(0)
    rows_own = rows_z()
    stage_d(0)
    arrived(half_block, "z1a")
    send(half(zm, s, f, 0), half(zm, s, f, 0), at_z(zp), "z2p", SMALL)
    arrived(half_block, "z1b")
    send(half(zp, s, f, 1), half(zp, s, f, 1), at_z(zm), "z2m", SMALL)
    arrived(half_block, "z1c")
    stage_a(1)
    arrived(half_block, "z1d")
    stage_a(2)
    stage_e(0)
    stage_f(0)
    stage_b(1)
    stage_b(2)
    stage_c(1)
    stage_c(2)
    stage_d(1)
    stage_d(2)
    rows_near(rows_own)
    arrived(half_block, "z2p")
    arrived(half_block, "z2m")
    stage_a(3)
    stage_e(1)
    stage_e(2)
    stage_g(0)
    stage_f(1)
    stage_f(2)
    stage_b(3)
    stage_c(3)
    rows_far()
    stage_d(3)
    rows_core_near()
    stage_g(1)
    stage_g(2)
    stage_e(3)
    rows_core_far()
    finish_near()
    mm_part((0, 1, 2), True)
    last_near()
    last_far()
    finish_far()
    mm_last()

    own_norm = jnp.sum(jnp.sum(norm_acc[...], axis=1, keepdims=True), axis=0, keepdims=True)
    plane = (y * 4 + x) * 2 + c
    red_a[plane] = jnp.broadcast_to(own_norm, (1, 128))

    @pl.loop(0, 31, unroll=31)
    def _(k):
        to = lax.rem(plane + 1 + lax.rem(k + 16, 31), 32)
        send(
            red_a.at[plane], red_a.at[plane],
            (to // 8, lax.rem(to // 2, 4), zh, lax.rem(to, 2), zl), "red_a", RED_A,
        )

    arrived(red_a.at[0:31], "red_a")
    z16 = zh * 4 + zl
    red_b[z16] = jnp.sum(red_a[...], axis=0)

    @pl.loop(0, 15, unroll=15)
    def _(k):
        to = lax.rem(z16 + 1 + lax.rem(k + 7, 15), 16)
        send(
            red_b.at[z16], red_b.at[z16], (y, x, to // 4, c, lax.rem(to, 4)), "red_b", RED_B
        )

    take(big.at[:, 0:3, 0:3, 0, 0], left.at[SMALL])
    take(big.at[:, 0:3, :, :, :, :, 0:640], left.at[GATHER])
    take(big.at[0], left.at[FORWARD])
    for zd in range(4):

        @pl.when(jnp.logical_not(jnp.logical_and(y == zl, zl == zd)))
        def _():
            take(rows2, out_sem.at[zd])

    take(red_a.at[0:31], left.at[RED_A])
    arrived(red_b.at[0:15], "red_b")
    n_out[...] = jnp.sum(red_b[...], axis=0)
    take(red_b.at[0:15], left.at[RED_B])
    assert len(places) == N_LANDED, len(places)


def scale_kernel(precond, ratio, norm, p_in, r_in, p_out, r_out, n_out, scaled, sem):
    copies = [
        pltpu.make_async_copy(precond.at[0:64], p_in, sem.at[0]),
        pltpu.make_async_copy(precond.at[64:128], p_out, sem.at[1]),
        pltpu.make_async_copy(norm, n_out, sem.at[6]),
    ]
    for copy in copies:
        copy.start()
    rescale = jnp.sqrt(2.0 * D * H / norm[0:1, 0:1])
    for k, (target, rows) in enumerate(((r_in, 0), (r_in, 32), (r_out, 64), (r_out, 96))):
        scaled[rows : rows + 32] = ratio[rows : rows + 32] * rescale
        copy = pltpu.make_async_copy(
            scaled.at[rows : rows + 32], target.at[pl.ds(rows % 64, 32)], sem.at[2 + k]
        )
        copy.start()
        copies.append(copy)
    for copy in copies:
        copy.wait()


def shards(*args):
    hbm = pl.BlockSpec(memory_space=pltpu.HBM)
    vmem = pl.BlockSpec(memory_space=pltpu.VMEM)
    dma = pltpu.SemaphoreType.DMA
    both = pltpu.VMEM((128, 2048), F32)
    precond, ratio, norm = pl.pallas_call(
        kernel,
        out_shape=(both, both, pltpu.VMEM((1, 128), F32)),
        in_specs=[hbm] * 4,
        out_specs=(vmem,) * 3,
        scratch_shapes=[
            pltpu.VMEM((4, 2048), BF),
            pltpu.VMEM((4, 2048), BF),
            pltpu.VMEM((4, 2048), BF),
            pltpu.VMEM((4, 2048), BF),
            pltpu.VMEM((2, 8, 2048), F32),
            pltpu.VMEM((4, 8, 512), BF),
            pltpu.VMEM((2, 8, 1024), BF),
            pltpu.VMEM((2, 4, 4, 4, 2, 8, 1024), BF),
            pltpu.VMEM((4, 8, 512), BF),
            pltpu.VMEM((4, 4, 8, 128), BF),
            pltpu.VMEM((2, 4, 4, 4, 8, 128), BF),
            pltpu.VMEM((4, 128, 256), BF),
            pltpu.VMEM((4, 128, 256), BF),
            pltpu.VMEM((128, 2048), F32),
            pltpu.VMEM((128, 2048), F32),
            pltpu.VMEM((8, TILE), F32),
            pltpu.VMEM((32, 1, 128), F32),
            pltpu.VMEM((16, 1, 128), F32),
            dma((4,)),
            dma((5,)),
            dma((N_LANDED,)),
            dma((4,)),
            pltpu.SemaphoreType.REGULAR((2,)),
        ],
        compiler_params=pltpu.CompilerParams(
            collective_id=0, has_side_effects=True, vmem_limit_bytes=K1_LIMIT
        ),
    )(*(pltpu.with_memory_space_constraint(v, pltpu.HBM) for v in args))
    half = jax.ShapeDtypeStruct((64, 2048), F32)
    *outs, norm = pl.pallas_call(
        scale_kernel,
        out_shape=(half, half, half, half, jax.ShapeDtypeStruct((1, 128), F32)),
        in_specs=[vmem] * 3,
        out_specs=(hbm,) * 5,
        scratch_shapes=[pltpu.VMEM((128, 2048), F32), dma((7,))],
        compiler_params=pltpu.CompilerParams(vmem_limit_bytes=8 * 1024 * 1024),
    )(*(pltpu.with_memory_space_constraint(v, pltpu.VMEM) for v in (precond, ratio, norm)))
    return (*outs, norm[0, 0])


def solution(mesh):
    torus = Mesh(mesh.devices.reshape(4, 4, 4, 2, mesh.shape["mp"]), AXES)
    placed = (P(DP, None), P(DP, "mp"), P(DP, "mp"), P(DP, "mp"))
    return jax.shard_map(
        shards,
        mesh=torus,
        in_specs=placed,
        out_specs=(P(DP, "mp"), P(DP, "mp"), P(DP, "mp"), P(DP, "mp"), P()),
        check_vma=False,
    )
```

```python
import jax
import jax.numpy as jnp
from jax import lax
from jax.experimental import pallas as pl
from jax.experimental.pallas import tpu as pltpu
from jax.sharding import Mesh
from jax.sharding import PartitionSpec as P

D = 8192
H = 8192
EXAMPLES = 512
DP = ("dp_0", "dp_1", "dp_2", "dp_3")
AXES = ("dp_0", "dp_1", "dp_2", "dp_3", "mp")
MESH = pl.DeviceIdType.MESH
BF = jnp.bfloat16
F32 = jnp.float32

DAMPING = 0.1
EXPONENT = 0.75

SMALL, GATHER, FORWARD, RED_A, RED_B = range(5)
N_LANDED = 49
TILE = 256
K1_LIMIT = 32 * 1024 * 1024


def mod4(a):
    return lax.rem(a, 4)


def kernel(
    li_hbm, pre_hbm, ha_hbm, oa_hbm,
    p_all, r_all, n_out,
    pre_v, ha_v, oa_v, li_v, stack, rows0, pair_src,
    big, rows1, rows2, rows3, lhs_t, lhs_sq, acc_g, acc_s, norm_acc, red_a, red_b,
    in_sem, left, landed, out_sem, hello_sem,
):
    y, x, zh, c, zl = (lax.axis_index(a) for a in AXES)
    d = 1 - c
    f = x * d + y * c
    s = y * d + x * c
    fp, fm, fo = mod4(f + 1), mod4(f + 3), mod4(f + 2)
    sp, sm, so = mod4(s + 1), mod4(s + 3), mod4(s + 2)
    zp, zm, zo = mod4(zh + 1), mod4(zh + 3), mod4(zh + 2)

    def at_f(fd):
        return (y * d + fd * c, fd * d + x * c, zh, c, zl)

    def at_s(sd):
        return (sd * d + y * c, x * d + sd * c, zh, c, zl)

    def at_z(zd, core=None):
        return (y, x, zd, c if core is None else core, zl)

    partner = (y, x, zh, d, zl)

    barrier = pltpu.get_barrier_semaphore()

    def tell(semaphore, device):
        pl.semaphore_signal(semaphore, inc=1, device_id=device, device_id_type=MESH)

    for core in (c, d):
        tell(barrier, at_z(zp, core))
        tell(barrier, at_z(zm, core))
    for k in (1, 2, 3):
        tell(barrier, (y, x, zh, c, mod4(zl + k)))
        tell(barrier, (mod4(y + k), x, zh, c, zl))
        tell(barrier, (y, mod4(x + k), zh, c, zl))
    tell(barrier, partner)

    loads = [
        pltpu.make_async_copy(pre_hbm, pre_v, in_sem.at[0]),
        pltpu.make_async_copy(ha_hbm, ha_v, in_sem.at[1]),
        pltpu.make_async_copy(oa_hbm, oa_v, in_sem.at[2]),
        pltpu.make_async_copy(
            li_hbm.at[:, pl.ds(pl.multiple_of(zl * 2048, 2048), 2048)], li_v, in_sem.at[3]
        ),
    ]
    for load in loads:
        load.start()
    for load in loads:
        load.wait()
    preact = pre_v[...].astype(F32)
    logistic = 1.0 / (1.0 + jnp.exp(-preact))
    hidden = (preact * logistic).astype(BF)
    adjoint = (ha_v[...].astype(F32) * logistic * (1.0 + preact * (1.0 - logistic))).astype(BF)
    stack[0, 0:4, :] = adjoint.astype(F32)
    stack[0, 4:8, :] = oa_v[...].astype(F32)
    stack[1, 0:4, :] = li_v[...].astype(F32)
    stack[1, 4:8, :] = hidden.astype(F32)
    pair_src[0] = stack[0, :, 0:1024].astype(BF)
    pair_src[1] = stack[0, :, 1024:2048].astype(BF)
    big[c, zh, y, x, c] = pair_src[c]
    for k in range(4):
        rows0[k] = stack[1, :, 512 * k : 512 * (k + 1)].astype(BF)

    pl.semaphore_wait(barrier, 14)

    places = {}

    def place(key):
        return landed.at[places.setdefault(key, len(places))]

    def send(src, dst, device, key, group):
        pltpu.make_async_remote_copy(
            src_ref=src, dst_ref=dst, send_sem=left.at[group], recv_sem=place(key),
            device_id=device, device_id_type=MESH,
        ).start()

    def take(ref, semaphore):
        pltpu.make_async_copy(ref, ref, semaphore).wait()

    def arrived(ref, key):
        take(ref, place(key))

    one = big.at[0, 0, 0, 0]
    half_block = big.at[0, 0, 0, 0, :, :, 0:512]

    def block(z, sd, fd):
        return big.at[c, z, sd * d + fd * c, fd * d + sd * c]

    def half(z, sd, fd, k):
        return big.at[c, z, sd * d + fd * c, fd * d + sd * c, :, :, pl.ds(512 * k, 512)]

    def z_pieces(zd, k, key):
        cols = pl.ds(512 * k, 512)
        for core in (c, d):
            send(
                pair_src.at[core, :, cols], big.at[core, zh, y, x, c, :, cols],
                at_z(zd, core), key, SMALL,
            )

    z_pieces(zp, 0, "z1a")
    z_pieces(zm, 1, "z1b")
    send(pair_src.at[d], big.at[d, zh, y, x, c], partner, "pair", SMALL)
    for k in (1, 2, 3):
        xd = mod4(x + k)
        send(rows0.at[xd], rows1.at[x], (y, xd, zh, c, zl), "row_x", SMALL)
    row_own = pltpu.make_async_copy(rows0.at[x], rows1.at[x], in_sem.at[0])
    row_own.start()
    z_pieces(zp, 1, "z1c")
    z_pieces(zm, 0, "z1d")
    tell(hello_sem.at[0], at_z(zp))
    for k in (1, 2, 3):
        tell(hello_sem.at[1], (mod4(y + k), x, zh, c, zl))

    def rows_z():
        arrived(rows1.at[0:3], "row_x")
        row_own.wait()
        pl.semaphore_wait(hello_sem.at[0], 1)
        for zd, key in ((zo, "row_z_far"), (zp, "row_z"), (zm, "row_z")):
            cols = pl.ds(pl.multiple_of(zd * 128, 128), 128)
            send(rows1.at[:, :, cols], rows2.at[zh], at_z(zd), key, SMALL)
        local = pltpu.make_async_copy(
            rows1.at[:, :, pl.ds(pl.multiple_of(zh * 128, 128), 128)], rows2.at[zh], in_sem.at[1]
        )
        local.start()
        return local

    def rows_y(planes, key):
        for zd in range(4):
            own = jnp.logical_and(y == zl, zl == zd)
            for z in planes:

                @pl.when(own)
                def _():
                    pltpu.make_async_copy(rows2.at[z], rows3.at[c, z, y], place(key)).start()

                @pl.when(jnp.logical_not(own))
                def _():
                    pltpu.make_async_remote_copy(
                        src_ref=rows2.at[z], dst_ref=rows3.at[c, z, y], send_sem=out_sem.at[zd],
                        recv_sem=place(key), device_id=(zl, x, zh, c, zd), device_id_type=MESH,
                    ).start()

    def rows_near(local):
        arrived(rows2.at[0:2], "row_z")
        local.wait()
        pl.semaphore_wait(hello_sem.at[1], 3)
        rows_y((zh, zm, zp), "row_y")

    def rows_far():
        arrived(rows2.at[0], "row_z_far")
        rows_y((zo,), "row_y_far")

    def rows_core_near():
        arrived(rows3.at[0, 0:3], "row_y")
        for z in (zh, zm, zp):
            send(rows3.at[c, z], rows3.at[c, z], partner, "row_core", SMALL)

    def rows_core_far():
        arrived(rows3.at[0, 0], "row_y_far")
        send(rows3.at[c, zo], rows3.at[c, zo], partner, "row_core_far", SMALL)

    slices = (zh, zm, zp, zo)
    routes = {0: "++--", 1: "++--", 2: "++--", 3: "****"}

    def s_key(k, j, side):
        relayed = {"+": 0, "-": 1}.get(routes[k][j])
        if relayed == side:
            return ("s1", k, j)
        return ("rest", k, 0)

    def far_key(k):
        return ("rest", k, 1 if k == 3 else 0)

    def forward(k, sd, fd):
        z = slices[k]
        send(block(z, sd, fd), block(z, sd, fd), partner, ("x", k), FORWARD)

    def both_s(k, j, fd):
        z = slices[k]
        send(block(z, s, fd), block(z, s, fd), at_s(sp), s_key(k, j, 0), GATHER)
        send(block(z, s, fd), block(z, s, fd), at_s(sm), s_key(k, j, 1), GATHER)
        if routes[k][j] == "*":
            send(block(z, s, fd), block(z, s, fd), at_s(so), far_key(k), GATHER)
        forward(k, s, fd)

    def relay(k, j, fd):
        if routes[k][j] == "*":
            return
        z = slices[k]
        arrived(one, ("s1", k, j))
        came, goes = (sm, sp) if routes[k][j] == "+" else (sp, sm)
        send(block(z, came, fd), block(z, came, fd), at_s(goes), far_key(k), GATHER)
        forward(k, came, fd)

    def stage_a(k):
        z = slices[k]
        send(block(z, s, f), block(z, s, f), at_f(fp), ("f1", k, 0), GATHER)
        send(block(z, s, f), block(z, s, f), at_f(fm), ("f1", k, 1), GATHER)
        both_s(k, 0, f)
        send(block(z, s, f), block(z, s, f), at_f(fo), ("f2", k), GATHER)

    def stage_b(k):
        arrived(one, ("f1", k, 0))
        both_s(k, 1, fm)
        arrived(one, ("f1", k, 1))
        both_s(k, 2, fp)

    def stage_c(k):
        relay(k, 0, f)

    def stage_d(k):
        arrived(one, ("f2", k))
        both_s(k, 3, fo)

    def stage_e(k):
        relay(k, 1, fm)
        relay(k, 2, fp)

    def stage_f(k):
        relay(k, 3, fo)

    def forward_near(k):
        for j, fd in enumerate((f, fm, fp, fo)):
            if routes[k][j] != "+":
                forward(k, sm, fd)
            if routes[k][j] != "-":
                forward(k, sp, fd)

    def stage_g(k):
        arrived(big.at[0, 0, 0:2], ("rest", k, 0))
        forward_near(k)
        for fd in (f, fm, fp, fo):
            forward(k, so, fd)

    def last_near():
        arrived(big.at[0, 0, 0:2], ("rest", 3, 0))
        forward_near(3)

    def last_far():
        arrived(big.at[0, 0, 0], ("rest", 3, 1))
        for fd in (f, fm, fp, fo):
            forward(3, so, fd)

    def finish_rows(z):
        row = lax.broadcasted_iota(jnp.int32, (256, 128), 0)
        lane = lax.broadcasted_iota(jnp.int32, (256, 128), 1)
        keep = lax.rem(row // 4, 2) == lane // 64
        straight = lane // 64 == c
        parts = [rows3[core, z].reshape(16, 8, 128).astype(F32) for core in range(2)]
        data = jnp.stack(parts, axis=1).reshape(256, 128)
        turned = pltpu.roll(data, 64, 1)
        t = jnp.transpose(jnp.where(keep, jnp.where(straight, data, turned), 0.0))
        lhs_t[z] = t.astype(BF)
        lhs_sq[z] = (t * t).astype(BF)

    def finish_near():
        arrived(rows3.at[0, 0:3], "row_core")

        @pl.loop(0, 3)
        def _(k):
            finish_rows(mod4(zh + k + 3))

    def finish_far():
        arrived(rows3.at[0, 0], "row_core_far")
        finish_rows(zo)

    def dots(zs, j):
        cols = pl.ds(pl.multiple_of(lax.rem(j, 4) * TILE, TILE), TILE)
        rights = [big[j // 4, z, :, :, :, :, cols].astype(F32).reshape(256, TILE) for z in zs]
        right = jnp.concatenate(rights, axis=0)
        left_t = jnp.concatenate([lhs_t[z] for z in zs], axis=1)
        left_sq = jnp.concatenate([lhs_sq[z] for z in zs], axis=1)
        grad = jnp.dot(left_t, right.astype(BF), preferred_element_type=F32)
        square = jnp.dot(left_sq, (right * right).astype(BF), preferred_element_type=F32)
        return grad, square

    def mm_part(ks, first):
        for k in ks:
            arrived(big.at[0, 0], ("x", k))

        @pl.loop(0, 8, unroll=8)
        def _(j):
            grad, square = dots([slices[k] for k in ks], j)
            wide = pl.ds(pl.multiple_of(j * TILE, TILE), TILE)
            if first:
                acc_g[:, wide] = grad
                acc_s[:, wide] = square
            else:
                acc_g[:, wide] += grad
                acc_s[:, wide] += square

    def mm_last():
        arrived(big.at[0, 0], ("x", 3))
        norm_acc[...] = jnp.zeros_like(norm_acc)

        @pl.loop(0, 8, unroll=8)
        def _(j):
            grad, square = dots([zo], j)
            wide = pl.ds(pl.multiple_of(j * TILE, TILE), TILE)
            grad = (acc_g[:, wide] + grad) * (1.0 / EXAMPLES)
            base = (acc_s[:, wide] + square) * (1.0 / EXAMPLES) + DAMPING
            power = EXPONENT * jnp.log(base)
            ratio = grad * jnp.exp(-power)
            p_all[:, wide] = jnp.exp(power)
            r_all[:, wide] = ratio
            norm_acc[...] += jnp.sum((grad * ratio).reshape(16, 8, TILE), axis=0)

    arrived(big.at[0, 0, 0, 0, 0], "pair")
    stage_a(0)
    stage_b(0)
    stage_c(0)
    rows_own = rows_z()
    stage_d(0)
    arrived(half_block, "z1a")
    send(half(zm, s, f, 0), half(zm, s, f, 0), at_z(zp), "z2p", SMALL)
    arrived(half_block, "z1b")
    send(half(zp, s, f, 1), half(zp, s, f, 1), at_z(zm), "z2m", SMALL)
    arrived(half_block, "z1c")
    stage_a(1)
    arrived(half_block, "z1d")
    stage_a(2)
    stage_e(0)
    stage_f(0)
    stage_b(1)
    stage_b(2)
    stage_c(1)
    stage_c(2)
    stage_d(1)
    stage_d(2)
    rows_near(rows_own)
    arrived(half_block, "z2p")
    arrived(half_block, "z2m")
    stage_a(3)
    stage_e(1)
    stage_e(2)
    stage_g(0)
    stage_f(1)
    stage_f(2)
    stage_b(3)
    stage_c(3)
    rows_far()
    stage_d(3)
    rows_core_near()
    stage_g(1)
    stage_g(2)
    stage_e(3)
    rows_core_far()
    finish_near()
    last_near()
    last_far()
    mm_part((0, 1, 2), True)
    finish_far()
    mm_last()

    own_norm = jnp.sum(jnp.sum(norm_acc[...], axis=1, keepdims=True), axis=0, keepdims=True)
    plane = (y * 4 + x) * 2 + c
    red_a[plane] = jnp.broadcast_to(own_norm, (1, 128))

    @pl.loop(0, 31, unroll=31)
    def _(k):
        to = lax.rem(plane + 1 + lax.rem(k + 16, 31), 32)
        send(
            red_a.at[plane], red_a.at[plane],
            (to // 8, lax.rem(to // 2, 4), zh, lax.rem(to, 2), zl), "red_a", RED_A,
        )

    arrived(red_a.at[0:31], "red_a")
    z16 = zh * 4 + zl
    red_b[z16] = jnp.sum(red_a[...], axis=0)

    @pl.loop(0, 15, unroll=15)
    def _(k):
        to = lax.rem(z16 + 1 + lax.rem(k + 7, 15), 16)
        send(
            red_b.at[z16], red_b.at[z16], (y, x, to // 4, c, lax.rem(to, 4)), "red_b", RED_B
        )

    take(big.at[:, 0:3, 0:3, 0, 0], left.at[SMALL])
    take(big.at[:, 0:3, :, :, :, :, 0:640], left.at[GATHER])
    take(big.at[0], left.at[FORWARD])
    for zd in range(4):

        @pl.when(jnp.logical_not(jnp.logical_and(y == zl, zl == zd)))
        def _():
            take(rows2, out_sem.at[zd])

    take(red_a.at[0:31], left.at[RED_A])
    arrived(red_b.at[0:15], "red_b")
    n_out[...] = jnp.sum(red_b[...], axis=0)
    take(red_b.at[0:15], left.at[RED_B])
    assert len(places) == N_LANDED, len(places)


def scale_kernel(precond, ratio, norm, p_in, r_in, p_out, r_out, n_out, scaled, sem):
    copies = [
        pltpu.make_async_copy(precond.at[0:64], p_in, sem.at[0]),
        pltpu.make_async_copy(precond.at[64:128], p_out, sem.at[1]),
        pltpu.make_async_copy(norm, n_out, sem.at[6]),
    ]
    for copy in copies:
        copy.start()
    rescale = jnp.sqrt(2.0 * D * H / norm[0:1, 0:1])
    for k, (target, rows) in enumerate(((r_in, 0), (r_in, 32), (r_out, 64), (r_out, 96))):
        scaled[rows : rows + 32] = ratio[rows : rows + 32] * rescale
        copy = pltpu.make_async_copy(
            scaled.at[rows : rows + 32], target.at[pl.ds(rows % 64, 32)], sem.at[2 + k]
        )
        copy.start()
        copies.append(copy)
    for copy in copies:
        copy.wait()


def shards(*args):
    hbm = pl.BlockSpec(memory_space=pltpu.HBM)
    vmem = pl.BlockSpec(memory_space=pltpu.VMEM)
    dma = pltpu.SemaphoreType.DMA
    both = pltpu.VMEM((128, 2048), F32)
    precond, ratio, norm = pl.pallas_call(
        kernel,
        out_shape=(both, both, pltpu.VMEM((1, 128), F32)),
        in_specs=[hbm] * 4,
        out_specs=(vmem,) * 3,
        scratch_shapes=[
            pltpu.VMEM((4, 2048), BF),
            pltpu.VMEM((4, 2048), BF),
            pltpu.VMEM((4, 2048), BF),
            pltpu.VMEM((4, 2048), BF),
            pltpu.VMEM((2, 8, 2048), F32),
            pltpu.VMEM((4, 8, 512), BF),
            pltpu.VMEM((2, 8, 1024), BF),
            pltpu.VMEM((2, 4, 4, 4, 2, 8, 1024), BF),
            pltpu.VMEM((4, 8, 512), BF),
            pltpu.VMEM((4, 4, 8, 128), BF),
            pltpu.VMEM((2, 4, 4, 4, 8, 128), BF),
            pltpu.VMEM((4, 128, 256), BF),
            pltpu.VMEM((4, 128, 256), BF),
            pltpu.VMEM((128, 2048), F32),
            pltpu.VMEM((128, 2048), F32),
            pltpu.VMEM((8, TILE), F32),
            pltpu.VMEM((32, 1, 128), F32),
            pltpu.VMEM((16, 1, 128), F32),
            dma((4,)),
            dma((5,)),
            dma((N_LANDED,)),
            dma((4,)),
            pltpu.SemaphoreType.REGULAR((2,)),
        ],
        compiler_params=pltpu.CompilerParams(
            collective_id=0, has_side_effects=True, vmem_limit_bytes=K1_LIMIT
        ),
    )(*(pltpu.with_memory_space_constraint(v, pltpu.HBM) for v in args))
    half = jax.ShapeDtypeStruct((64, 2048), F32)
    *outs, norm = pl.pallas_call(
        scale_kernel,
        out_shape=(half, half, half, half, jax.ShapeDtypeStruct((1, 128), F32)),
        in_specs=[vmem] * 3,
        out_specs=(hbm,) * 5,
        scratch_shapes=[pltpu.VMEM((128, 2048), F32), dma((7,))],
        compiler_params=pltpu.CompilerParams(vmem_limit_bytes=8 * 1024 * 1024),
    )(*(pltpu.with_memory_space_constraint(v, pltpu.VMEM) for v in (precond, ratio, norm)))
    return (*outs, norm[0, 0])


def solution(mesh):
    torus = Mesh(mesh.devices.reshape(4, 4, 4, 2, mesh.shape["mp"]), AXES)
    placed = (P(DP, None), P(DP, "mp"), P(DP, "mp"), P(DP, "mp"))
    return jax.shard_map(
        shards,
        mesh=torus,
        in_specs=placed,
        out_specs=(P(DP, "mp"), P(DP, "mp"), P(DP, "mp"), P(DP, "mp"), P()),
        check_vma=False,
    )
```

```python
import jax
import jax.numpy as jnp
from jax import lax
from jax.experimental import pallas as pl
from jax.experimental.pallas import tpu as pltpu
from jax.sharding import Mesh
from jax.sharding import PartitionSpec as P

D = 8192
H = 8192
EXAMPLES = 512
DP = ("dp_0", "dp_1", "dp_2", "dp_3")
AXES = ("dp_0", "dp_1", "dp_2", "dp_3", "mp")
MESH = pl.DeviceIdType.MESH
BF = jnp.bfloat16
F32 = jnp.float32

DAMPING = 0.1
EXPONENT = 0.75

SMALL, GATHER, FORWARD, RED_A, RED_B = range(5)
N_LANDED = 49
TILE = 256
K1_LIMIT = 32 * 1024 * 1024


def mod4(a):
    return lax.rem(a, 4)


def kernel(
    li_hbm, pre_hbm, ha_hbm, oa_hbm,
    p_all, r_all, n_out,
    pre_v, ha_v, oa_v, li_v, stack, rows0, pair_src,
    big, rows1, rows2, rows3, lhs_t, lhs_sq, acc_g, acc_s, norm_acc, red_a, red_b,
    in_sem, left, landed, out_sem, hello_sem,
):
    y, x, zh, c, zl = (lax.axis_index(a) for a in AXES)
    d = 1 - c
    f = x * d + y * c
    s = y * d + x * c
    fp, fm, fo = mod4(f + 1), mod4(f + 3), mod4(f + 2)
    sp, sm, so = mod4(s + 1), mod4(s + 3), mod4(s + 2)
    zp, zm, zo = mod4(zh + 1), mod4(zh + 3), mod4(zh + 2)

    def at_f(fd):
        return (y * d + fd * c, fd * d + x * c, zh, c, zl)

    def at_s(sd):
        return (sd * d + y * c, x * d + sd * c, zh, c, zl)

    def at_z(zd, core=None):
        return (y, x, zd, c if core is None else core, zl)

    partner = (y, x, zh, d, zl)

    barrier = pltpu.get_barrier_semaphore()

    def tell(semaphore, device):
        pl.semaphore_signal(semaphore, inc=1, device_id=device, device_id_type=MESH)

    for core in (c, d):
        tell(barrier, at_z(zp, core))
        tell(barrier, at_z(zm, core))
    for k in (1, 2, 3):
        tell(barrier, (y, x, zh, c, mod4(zl + k)))
        tell(barrier, (mod4(y + k), x, zh, c, zl))
        tell(barrier, (y, mod4(x + k), zh, c, zl))
    tell(barrier, partner)

    loads = [
        pltpu.make_async_copy(pre_hbm, pre_v, in_sem.at[0]),
        pltpu.make_async_copy(ha_hbm, ha_v, in_sem.at[1]),
        pltpu.make_async_copy(oa_hbm, oa_v, in_sem.at[2]),
        pltpu.make_async_copy(
            li_hbm.at[:, pl.ds(pl.multiple_of(zl * 2048, 2048), 2048)], li_v, in_sem.at[3]
        ),
    ]
    for load in loads:
        load.start()
    for load in loads:
        load.wait()
    preact = pre_v[...].astype(F32)
    logistic = 1.0 / (1.0 + jnp.exp(-preact))
    hidden = (preact * logistic).astype(BF)
    adjoint = (ha_v[...].astype(F32) * logistic * (1.0 + preact * (1.0 - logistic))).astype(BF)
    stack[0, 0:4, :] = adjoint.astype(F32)
    stack[0, 4:8, :] = oa_v[...].astype(F32)
    stack[1, 0:4, :] = li_v[...].astype(F32)
    stack[1, 4:8, :] = hidden.astype(F32)
    pair_src[0] = stack[0, :, 0:1024].astype(BF)
    pair_src[1] = stack[0, :, 1024:2048].astype(BF)
    big[c, zh, y, x, c] = pair_src[c]
    for k in range(4):
        rows0[k] = stack[1, :, 512 * k : 512 * (k + 1)].astype(BF)

    pl.semaphore_wait(barrier, 14)

    places = {}

    def place(key):
        return landed.at[places.setdefault(key, len(places))]

    def send(src, dst, device, key, group):
        pltpu.make_async_remote_copy(
            src_ref=src, dst_ref=dst, send_sem=left.at[group], recv_sem=place(key),
            device_id=device, device_id_type=MESH,
        ).start()

    def take(ref, semaphore):
        pltpu.make_async_copy(ref, ref, semaphore).wait()

    def arrived(ref, key):
        take(ref, place(key))

    one = big.at[0, 0, 0, 0]
    half_block = big.at[0, 0, 0, 0, :, :, 0:512]

    def block(z, sd, fd):
        return big.at[c, z, sd * d + fd * c, fd * d + sd * c]

    def half(z, sd, fd, k):
        return big.at[c, z, sd * d + fd * c, fd * d + sd * c, :, :, pl.ds(512 * k, 512)]

    def z_pieces(zd, k, key):
        cols = pl.ds(512 * k, 512)
        for core in (c, d):
            send(
                pair_src.at[core, :, cols], big.at[core, zh, y, x, c, :, cols],
                at_z(zd, core), key, SMALL,
            )

    z_pieces(zp, 0, "z1a")
    z_pieces(zm, 1, "z1b")
    send(pair_src.at[d], big.at[d, zh, y, x, c], partner, "pair", SMALL)
    for k in (1, 2, 3):
        xd = mod4(x + k)
        send(rows0.at[xd], rows1.at[x], (y, xd, zh, c, zl), "row_x", SMALL)
    row_own = pltpu.make_async_copy(rows0.at[x], rows1.at[x], in_sem.at[0])
    row_own.start()
    z_pieces(zp, 1, "z1c")
    z_pieces(zm, 0, "z1d")
    tell(hello_sem.at[0], at_z(zp))
    for k in (1, 2, 3):
        tell(hello_sem.at[1], (mod4(y + k), x, zh, c, zl))

    def rows_z():
        arrived(rows1.at[0:3], "row_x")
        row_own.wait()
        pl.semaphore_wait(hello_sem.at[0], 1)
        for zd, key in ((zo, "row_z_far"), (zp, "row_z"), (zm, "row_z")):
            cols = pl.ds(pl.multiple_of(zd * 128, 128), 128)
            send(rows1.at[:, :, cols], rows2.at[zh], at_z(zd), key, SMALL)
        local = pltpu.make_async_copy(
            rows1.at[:, :, pl.ds(pl.multiple_of(zh * 128, 128), 128)], rows2.at[zh], in_sem.at[1]
        )
        local.start()
        return local

    def rows_y(planes, key):
        for zd in range(4):
            own = jnp.logical_and(y == zl, zl == zd)
            for z in planes:

                @pl.when(own)
                def _():
                    pltpu.make_async_copy(rows2.at[z], rows3.at[c, z, y], place(key)).start()

                @pl.when(jnp.logical_not(own))
                def _():
                    pltpu.make_async_remote_copy(
                        src_ref=rows2.at[z], dst_ref=rows3.at[c, z, y], send_sem=out_sem.at[zd],
                        recv_sem=place(key), device_id=(zl, x, zh, c, zd), device_id_type=MESH,
                    ).start()

    def rows_near(local):
        arrived(rows2.at[0:2], "row_z")
        local.wait()
        pl.semaphore_wait(hello_sem.at[1], 3)
        rows_y((zh, zm, zp), "row_y")

    def rows_far():
        arrived(rows2.at[0], "row_z_far")
        rows_y((zo,), "row_y_far")

    def rows_core_near():
        arrived(rows3.at[0, 0:3], "row_y")
        for z in (zh, zm, zp):
            send(rows3.at[c, z], rows3.at[c, z], partner, "row_core", SMALL)

    def rows_core_far():
        arrived(rows3.at[0, 0], "row_y_far")
        send(rows3.at[c, zo], rows3.at[c, zo], partner, "row_core_far", SMALL)

    slices = (zh, zm, zp, zo)
    routes = {0: "++--", 1: "++--", 2: "++--", 3: "****"}

    def s_key(k, j, side):
        relayed = {"+": 0, "-": 1}.get(routes[k][j])
        if relayed == side:
            return ("s1", k, j)
        return ("rest", k, 0)

    def far_key(k):
        return ("rest", k, 1 if k == 3 else 0)

    def forward(k, sd, fd):
        z = slices[k]
        send(block(z, sd, fd), block(z, sd, fd), partner, ("x", k), FORWARD)

    def both_s(k, j, fd):
        z = slices[k]
        send(block(z, s, fd), block(z, s, fd), at_s(sp), s_key(k, j, 0), GATHER)
        send(block(z, s, fd), block(z, s, fd), at_s(sm), s_key(k, j, 1), GATHER)
        if routes[k][j] == "*":
            send(block(z, s, fd), block(z, s, fd), at_s(so), far_key(k), GATHER)
        forward(k, s, fd)

    def relay(k, j, fd):
        if routes[k][j] == "*":
            return
        z = slices[k]
        arrived(one, ("s1", k, j))
        came, goes = (sm, sp) if routes[k][j] == "+" else (sp, sm)
        send(block(z, came, fd), block(z, came, fd), at_s(goes), far_key(k), GATHER)
        forward(k, came, fd)

    def stage_a(k):
        z = slices[k]
        send(block(z, s, f), block(z, s, f), at_f(fp), ("f1", k, 0), GATHER)
        send(block(z, s, f), block(z, s, f), at_f(fm), ("f1", k, 1), GATHER)
        both_s(k, 0, f)
        send(block(z, s, f), block(z, s, f), at_f(fo), ("f2", k), GATHER)

    def stage_b(k):
        arrived(one, ("f1", k, 0))
        both_s(k, 1, fm)
        arrived(one, ("f1", k, 1))
        both_s(k, 2, fp)

    def stage_c(k):
        relay(k, 0, f)

    def stage_d(k):
        arrived(one, ("f2", k))
        both_s(k, 3, fo)

    def stage_e(k):
        relay(k, 1, fm)
        relay(k, 2, fp)

    def stage_f(k):
        relay(k, 3, fo)

    def forward_near(k):
        for j, fd in enumerate((f, fm, fp, fo)):
            if routes[k][j] != "+":
                forward(k, sm, fd)
            if routes[k][j] != "-":
                forward(k, sp, fd)

    def stage_g(k):
        arrived(big.at[0, 0, 0:2], ("rest", k, 0))
        forward_near(k)
        for fd in (f, fm, fp, fo):
            forward(k, so, fd)

    def last_near():
        arrived(big.at[0, 0, 0:2], ("rest", 3, 0))
        forward_near(3)

    def last_far():
        arrived(big.at[0, 0, 0], ("rest", 3, 1))
        for fd in (f, fm, fp, fo):
            forward(3, so, fd)

    def finish_rows(z):
        row = lax.broadcasted_iota(jnp.int32, (256, 128), 0)
        lane = lax.broadcasted_iota(jnp.int32, (256, 128), 1)
        keep = lax.rem(row // 4, 2) == lane // 64
        straight = lane // 64 == c
        parts = [rows3[core, z].reshape(16, 8, 128).astype(F32) for core in range(2)]
        data = jnp.stack(parts, axis=1).reshape(256, 128)
        turned = pltpu.roll(data, 64, 1)
        t = jnp.transpose(jnp.where(keep, jnp.where(straight, data, turned), 0.0))
        lhs_t[z] = t.astype(BF)
        lhs_sq[z] = (t * t).astype(BF)

    def finish_near():
        arrived(rows3.at[0, 0:3], "row_core")

        @pl.loop(0, 3)
        def _(k):
            finish_rows(mod4(zh + k + 3))

    def finish_far():
        arrived(rows3.at[0, 0], "row_core_far")
        finish_rows(zo)

    def dots(zs, j):
        cols = pl.ds(pl.multiple_of(lax.rem(j, 4) * TILE, TILE), TILE)
        rights = [big[j // 4, z, :, :, :, :, cols].astype(F32).reshape(256, TILE) for z in zs]
        right = jnp.concatenate(rights, axis=0)
        left_t = jnp.concatenate([lhs_t[z] for z in zs], axis=1)
        left_sq = jnp.concatenate([lhs_sq[z] for z in zs], axis=1)
        grad = jnp.dot(left_t, right.astype(BF), preferred_element_type=F32)
        square = jnp.dot(left_sq, (right * right).astype(BF), preferred_element_type=F32)
        return grad, square

    def mm_part(ks, first):
        for k in ks:
            arrived(big.at[0, 0], ("x", k))

        @pl.loop(0, 8, unroll=8)
        def _(j):
            grad, square = dots([slices[k] for k in ks], j)
            wide = pl.ds(pl.multiple_of(j * TILE, TILE), TILE)
            if first:
                acc_g[:, wide] = grad
                acc_s[:, wide] = square
            else:
                acc_g[:, wide] += grad
                acc_s[:, wide] += square

    def mm_last():
        arrived(big.at[0, 0], ("x", 3))
        norm_acc[...] = jnp.zeros_like(norm_acc)

        @pl.loop(0, 8, unroll=8)
        def _(j):
            grad, square = dots([zo], j)
            wide = pl.ds(pl.multiple_of(j * TILE, TILE), TILE)
            grad = (acc_g[:, wide] + grad) * (1.0 / EXAMPLES)
            base = (acc_s[:, wide] + square) * (1.0 / EXAMPLES) + DAMPING
            power = EXPONENT * jnp.log(base)
            ratio = grad * jnp.exp(-power)
            p_all[:, wide] = jnp.exp(power)
            r_all[:, wide] = ratio
            norm_acc[...] += jnp.sum((grad * ratio).reshape(16, 8, TILE), axis=0)

    arrived(big.at[0, 0, 0, 0, 0], "pair")
    stage_a(0)
    stage_b(0)
    stage_c(0)
    rows_own = rows_z()
    stage_d(0)
    arrived(half_block, "z1a")
    send(half(zm, s, f, 0), half(zm, s, f, 0), at_z(zp), "z2p", SMALL)
    arrived(half_block, "z1b")
    send(half(zp, s, f, 1), half(zp, s, f, 1), at_z(zm), "z2m", SMALL)
    arrived(half_block, "z1c")
    stage_a(1)
    arrived(half_block, "z1d")
    stage_a(2)
    stage_e(0)
    stage_f(0)
    stage_b(1)
    stage_b(2)
    stage_c(1)
    stage_c(2)
    stage_d(1)
    stage_d(2)
    rows_near(rows_own)
    arrived(half_block, "z2p")
    arrived(half_block, "z2m")
    stage_a(3)
    stage_e(1)
    stage_e(2)
    stage_g(0)
    @pl.when(c == 0)
    def _():
        stage_b(3)
        stage_f(1)
        stage_f(2)

    @pl.when(c == 1)
    def _():
        stage_f(1)
        stage_f(2)
        stage_b(3)

    stage_c(3)
    rows_far()
    stage_d(3)
    rows_core_near()
    stage_g(1)
    stage_g(2)
    stage_e(3)
    rows_core_far()
    finish_near()
    last_near()
    last_far()
    mm_part((0, 1, 2), True)
    finish_far()
    mm_last()

    own_norm = jnp.sum(jnp.sum(norm_acc[...], axis=1, keepdims=True), axis=0, keepdims=True)
    plane = (y * 4 + x) * 2 + c
    red_a[plane] = jnp.broadcast_to(own_norm, (1, 128))

    @pl.loop(0, 31, unroll=31)
    def _(k):
        to = lax.rem(plane + 1 + lax.rem(k + 16, 31), 32)
        send(
            red_a.at[plane], red_a.at[plane],
            (to // 8, lax.rem(to // 2, 4), zh, lax.rem(to, 2), zl), "red_a", RED_A,
        )

    arrived(red_a.at[0:31], "red_a")
    z16 = zh * 4 + zl
    red_b[z16] = jnp.sum(red_a[...], axis=0)

    @pl.loop(0, 15, unroll=15)
    def _(k):
        to = lax.rem(z16 + 1 + lax.rem(k + 7, 15), 16)
        send(
            red_b.at[z16], red_b.at[z16], (y, x, to // 4, c, lax.rem(to, 4)), "red_b", RED_B
        )

    take(big.at[:, 0:3, 0:3, 0, 0], left.at[SMALL])
    take(big.at[:, 0:3, :, :, :, :, 0:640], left.at[GATHER])
    take(big.at[0], left.at[FORWARD])
    for zd in range(4):

        @pl.when(jnp.logical_not(jnp.logical_and(y == zl, zl == zd)))
        def _():
            take(rows2, out_sem.at[zd])

    take(red_a.at[0:31], left.at[RED_A])
    arrived(red_b.at[0:15], "red_b")
    n_out[...] = jnp.sum(red_b[...], axis=0)
    take(red_b.at[0:15], left.at[RED_B])
    assert len(places) == N_LANDED, len(places)


def scale_kernel(precond, ratio, norm, p_in, r_in, p_out, r_out, n_out, scaled, sem):
    copies = [
        pltpu.make_async_copy(precond.at[0:64], p_in, sem.at[0]),
        pltpu.make_async_copy(precond.at[64:128], p_out, sem.at[1]),
        pltpu.make_async_copy(norm, n_out, sem.at[6]),
    ]
    for copy in copies:
        copy.start()
    rescale = jnp.sqrt(2.0 * D * H / norm[0:1, 0:1])
    for k, (target, rows) in enumerate(((r_in, 0), (r_in, 32), (r_out, 64), (r_out, 96))):
        scaled[rows : rows + 32] = ratio[rows : rows + 32] * rescale
        copy = pltpu.make_async_copy(
            scaled.at[rows : rows + 32], target.at[pl.ds(rows % 64, 32)], sem.at[2 + k]
        )
        copy.start()
        copies.append(copy)
    for copy in copies:
        copy.wait()


def shards(*args):
    hbm = pl.BlockSpec(memory_space=pltpu.HBM)
    vmem = pl.BlockSpec(memory_space=pltpu.VMEM)
    dma = pltpu.SemaphoreType.DMA
    both = pltpu.VMEM((128, 2048), F32)
    precond, ratio, norm = pl.pallas_call(
        kernel,
        out_shape=(both, both, pltpu.VMEM((1, 128), F32)),
        in_specs=[hbm] * 4,
        out_specs=(vmem,) * 3,
        scratch_shapes=[
            pltpu.VMEM((4, 2048), BF),
            pltpu.VMEM((4, 2048), BF),
            pltpu.VMEM((4, 2048), BF),
            pltpu.VMEM((4, 2048), BF),
            pltpu.VMEM((2, 8, 2048), F32),
            pltpu.VMEM((4, 8, 512), BF),
            pltpu.VMEM((2, 8, 1024), BF),
            pltpu.VMEM((2, 4, 4, 4, 2, 8, 1024), BF),
            pltpu.VMEM((4, 8, 512), BF),
            pltpu.VMEM((4, 4, 8, 128), BF),
            pltpu.VMEM((2, 4, 4, 4, 8, 128), BF),
            pltpu.VMEM((4, 128, 256), BF),
            pltpu.VMEM((4, 128, 256), BF),
            pltpu.VMEM((128, 2048), F32),
            pltpu.VMEM((128, 2048), F32),
            pltpu.VMEM((8, TILE), F32),
            pltpu.VMEM((32, 1, 128), F32),
            pltpu.VMEM((16, 1, 128), F32),
            dma((4,)),
            dma((5,)),
            dma((N_LANDED,)),
            dma((4,)),
            pltpu.SemaphoreType.REGULAR((2,)),
        ],
        compiler_params=pltpu.CompilerParams(
            collective_id=0, has_side_effects=True, vmem_limit_bytes=K1_LIMIT
        ),
    )(*(pltpu.with_memory_space_constraint(v, pltpu.HBM) for v in args))
    half = jax.ShapeDtypeStruct((64, 2048), F32)
    *outs, norm = pl.pallas_call(
        scale_kernel,
        out_shape=(half, half, half, half, jax.ShapeDtypeStruct((1, 128), F32)),
        in_specs=[vmem] * 3,
        out_specs=(hbm,) * 5,
        scratch_shapes=[pltpu.VMEM((128, 2048), F32), dma((7,))],
        compiler_params=pltpu.CompilerParams(vmem_limit_bytes=8 * 1024 * 1024),
    )(*(pltpu.with_memory_space_constraint(v, pltpu.VMEM) for v in (precond, ratio, norm)))
    return (*outs, norm[0, 0])


def solution(mesh):
    torus = Mesh(mesh.devices.reshape(4, 4, 4, 2, mesh.shape["mp"]), AXES)
    placed = (P(DP, None), P(DP, "mp"), P(DP, "mp"), P(DP, "mp"))
    return jax.shard_map(
        shards,
        mesh=torus,
        in_specs=placed,
        out_specs=(P(DP, "mp"), P(DP, "mp"), P(DP, "mp"), P(DP, "mp"), P()),
        check_vma=False,
    )
```
